32 devices in a mesh: pair: 8 (over y, x, core), ga: 4 (over z).
Axes of the slice: x: 2, y: 2, z: 4, core: 2. Of those that a mesh axis runs over, the one named last changes fastest.
Arguments:
- densities: bfloat16 [12288, 4096], P('pair', 'ga'), may hold values from -6 to 6
- val_band: int32 [12288], P('pair'), may hold values from 0 to 127
- cond_band: int32 [12288], P('pair'), may hold values from 0 to 255
- val_energy: float32 [128], replicated, may hold values from -12 to -1
- cond_energy: float32 [256], replicated, may hold values from 1 to 12
Outputs:
- chi: float32 [4096, 4096], P('ga', 'pair')
The draws below stay inside these ranges and needn't reach their ends.
All inputs are finite; a program needn't handle non-finite values.
Results may differ from the reference program's by a relative error of at most 0.0012.
Values may be sent and summed in bfloat16 or wider, within the bound.
A program may use at most 128 MiB of HBM per device.

```python
import math
import jax
import jax.numpy as jnp
from jax import lax

NG = 4096
NV = 128
NC = 256
P_DEV = 1536
PAIRS = 12288
N_PAIR = 8


def place_ends(array, stream_key, least, top_value):
    shape = array.shape
    index_at = [jax.random.randint(jax.random.fold_in(stream_key, axis), (), 0, shape[axis]) for axis in range(len(shape))]
    array = array.at[tuple(index_at)].set(least)
    longest = shape.index(max(shape))
    index_at[longest] = (index_at[longest] + 1) % shape[longest]
    return array.at[tuple(index_at)].set(top_value)


def steps_of(stream_key, shape, cuts, least, high):
    gain, own = 1.0, jax.random.fold_in(stream_key, 6)
    for axis_at, shards_of in cuts:
        heights = jnp.exp(jax.random.uniform(jax.random.fold_in(own, axis_at), (shards_of,), jnp.float32, least / len(cuts), high / len(cuts)))
        gain = gain * jnp.repeat(heights, shape[axis_at] // shards_of).reshape([-1 if axis == axis_at else 1 for axis in range(len(shape))])
    return gain


def gaussian(rng, shape, scale, most, shards=(), held_as=jnp.bfloat16):
    level = steps_of(rng, shape, shards, -0.22, 0.18) if shards else 1.0
    entries = jax.random.normal(rng, shape, jnp.float32) * scale * level
    return jnp.minimum(jnp.maximum(entries, -most), most).astype(held_as)


def setup_inputs(seed: int = 0) -> dict:
    arg_keys = jax.random.split(jax.random.key(seed), 6)
    return {
        "densities": gaussian(arg_keys[0], (PAIRS, NG), 1.0, 6.0, ((0, 8), (1, 4))),
        "val_band": place_ends(jax.random.randint(arg_keys[1], (PAIRS,), 0, NV), jax.random.fold_in(arg_keys[1], 1), 0, NV - 1).astype(jnp.int32),
        "cond_band": place_ends(jax.random.randint(arg_keys[2], (PAIRS,), 0, NC), jax.random.fold_in(arg_keys[2], 1), 0, NC - 1).astype(jnp.int32),
        "val_energy": jnp.clip(jax.random.uniform(arg_keys[3], (NV,), jnp.float32, -12.0, -1.0), -12.0, -1.0),
        "cond_energy": jnp.clip(jax.random.uniform(arg_keys[4], (NC,), jnp.float32, 1.0, 12.0), 1.0, 12.0),
    }


def reference(densities, val_band, cond_band, val_energy, cond_energy):
    gap = val_energy[val_band] - cond_energy[cond_band]
    weight = 4.0 / (gap * math.sqrt(PAIRS))
    scaled = (weight[:, None] * densities.astype(jnp.float32)).astype(jnp.bfloat16)
    left_groups = scaled.reshape(N_PAIR, P_DEV, NG)
    right_groups = densities.reshape(N_PAIR, P_DEV, NG)

    def add_group(total, pieces):
        left, right = pieces
        partial_value = lax.dot_general(left, right, (((0,), (0,)), ((), ())), preferred_element_type=jnp.float32)
        return (total + partial_value, None)
    total, unused = lax.scan(add_group, jnp.zeros((NG, NG), jnp.float32), (left_groups, right_groups))
    return total
```

```python
import functools
import math

import jax
import jax.numpy as jnp
from jax import lax
from jax.experimental import pallas as pl
from jax.experimental.pallas import tpu as pltpu
from jax.sharding import PartitionSpec as P

MESH = pl.DeviceIdType.MESH
PLANES, SQUARE = 4, 2
F32, BF16, I16 = jnp.float32, jnp.bfloat16, jnp.int16


def lookup(bands, table):
    levels = lax.broadcasted_iota(jnp.int32, (1, table.shape[0]), 1)
    onehot = (bands[:, None] == levels).astype(jnp.float32)
    return jnp.sum(onehot * table[None, :], axis=1)


def weights(densities, val_band, cond_band, val_energy, cond_energy):
    pairs_total = densities.shape[0] * lax.axis_size("pair")
    gap = lookup(val_band, val_energy) - lookup(cond_band, cond_energy)
    return 4.0 / (gap * math.sqrt(pairs_total))


def scale(weight, block):
    return (weight[:, None] * block.astype(jnp.float32)).astype(jnp.bfloat16)


def contract(left, right):
    return lax.dot_general(
        left, right, (((0,), (0,)), ((), ())), preferred_element_type=jnp.float32
    )


def gather_all(densities, *bands):
    scaled = scale(weights(densities, *bands), densities)
    gathered = lax.all_gather(densities, "ga", axis=1, tiled=True)
    owned = lax.psum_scatter(
        contract(gathered, scaled), "pair", scatter_dimension=0, tiled=True
    )
    return owned.T


STEPS, LOW = 816.0, -27.0


def encode(x):
    t = jnp.log(jnp.abs(x)) * (STEPS / math.log(2)) + (1.5 - LOW * STEPS)
    t = jnp.maximum(t, 0.0).astype(jnp.int32)
    return jnp.where(x < 0, -t, t).astype(I16)


def decode(code):
    c = code.astype(jnp.int32).astype(F32)
    m = jnp.exp2(jnp.abs(c) * (1 / STEPS) + (LOW - 1 / STEPS))
    return jnp.where(c < 0, -m, m)


TILES = (
    (0, 1, 1), (0, 0, 1), (0, 2, 0), (0, 3, 0),
    (2, 1, 0), (2, 0, 0), (3, 1, 0), (3, 0, 0),
    (1, 0, 1), (1, 2, 0), (1, 3, 0),
)
INWARD = ((0, 0), (0, 1), (1, 0), (1, 1), (0, 2), (1, 2), (1, 3), (0, 3))
ARRIVALS = 8
RING = 4


def chunk_slot(block, k, full):
    if block == 0:
        return 0
    if block == 1:
        slots = [INWARD.index((0, k)) + 1]
        if full:
            slots.append(INWARD.index((1, k)) + 1)
        return max(slots)
    return (block - 2) * 4 + k + 1


def piece_slot(tile, k, ch):
    a, b, full = TILES[tile]
    columns = max(chunk_slot(b, 2 * ch, full), chunk_slot(b, 2 * ch + 1, full))
    return max(chunk_slot(a, k, full), columns)


PRIORITY = (6, 7, 4, 5, 10, 9, 8, 3, 0, 2, 1)
PIECES = sorted(
    ((t, k, ch) for t in range(11) for k in range(4) for ch in range(2)),
    key=lambda p: (piece_slot(*p), PRIORITY.index(p[0]), p[1], p[2]),
)
LAST = ARRIVALS + 4


def ranges(slots):
    slots = sorted(slots)
    return [sum(1 for s in slots if s < n) for n in range(LAST + 2)]


def order(items, slot):
    items = sorted(items, key=lambda i: (slot(*i), i))
    return items, ranges([slot(*i) for i in items])


def yd_slot(j, kk):
    return max(piece_slot(4 + j, 2 * v + kk, ch) for v in (0, 1) for ch in (0, 1)) + 1


def xd_slot(t, kk):
    return max(yd_slot(2 * t + x, kk) for x in (0, 1)) + 1


def xt_slot(k):
    return max(piece_slot(j, k, ch) for j in range(4) for ch in (0, 1)) + 1


YD, YD_AT = order([(j, kk) for j in range(4) for kk in range(2)], yd_slot)
XD, XD_AT = order([(t, kk) for t in range(2) for kk in range(2)], xd_slot)
PIECE_AT = ranges([piece_slot(*p) for p in PIECES])
G_ORDER = []
for p in PIECES:
    if p[0] >= 8 and (p[0] - 7, p[1]) not in G_ORDER:
        G_ORDER.append((p[0] - 7, p[1]))


def pick(index, values):
    result = jnp.int32(values[0])
    for n, value in enumerate(values):
        if n and value != values[0]:
            result = jnp.where(index == n, value, result)
    return result


def many(start, stop, body):
    def step(n, carry):
        body(n)
        return carry

    lax.fori_loop(start, stop, step, 0)


def kernel(
    dens, weight, out, mb, st, drecv, dsend, acc, keep, keepd, xr, yr, yrd, xrd, din, dfw,
    load_sem, in_s, in_r, mid_s, mid_r, p_s, p_r, xt_s, xt_r, yt_s, yt_r,
    yd_s, yd_r, xd_s, xd_r, zd_s, zd_r, fw_s, fw_r, g_s, g_r,
):
    pair, z = lax.axis_index("pair"), lax.axis_index("ga")
    c = pair % 2
    x = (pair // 2) % 2
    y = pair // 4
    h = z // 2
    X = (x + h) % 2
    Y = (y + h) % 2
    inner = (z == 1) | (z == 2)
    outer = (z == 0) | (z == 3)

    pairs, width = dens.shape
    half = pairs // 2
    rb = width // 4
    hw = width // 2
    kb = 256 if half % 256 == 0 else half
    keep_off = h * half
    give_off = (1 - h) * half

    def at(yy, xx, cc, zz):
        return ((yy * SQUARE + xx) * 2 + cc, zz)

    to_core = at(y, x, 1 - c, z)
    to_x = at(y, 1 - x, c, z)
    to_y = at(1 - y, x, c, z)
    z_mate = z + 1 - 2 * (z % 2)
    z_cross = 3 - z
    to_mate = at(y, x, c, z_mate)
    to_cross = at(y, x, c, z_cross)

    def remote(src, dst, send, recv, to):
        return pltpu.make_async_remote_copy(
            src_ref=src, dst_ref=dst, send_sem=send, recv_sem=recv,
            device_id=to, device_id_type=MESH,
        )

    def rows(k, size=rb):
        return pl.ds(pl.multiple_of(k * size, size), size)

    def part(off):
        return pl.ds(pl.multiple_of(off, half), half)

    def columns(k):
        return pl.ds(pl.multiple_of(k * rb, rb), rb)

    def sides(k):
        return pl.ds(pl.multiple_of(k * hw, hw), hw)

    barrier = pltpu.get_barrier_semaphore()
    for to in (to_core, to_x, to_y, to_mate):
        pl.semaphore_signal(barrier, inc=1, device_id=to, device_id_type=MESH)

    @pl.when(inner)
    def _():
        pl.semaphore_signal(barrier, inc=1, device_id=to_cross, device_id_type=MESH)
        pl.semaphore_wait(barrier, 5)

    @pl.when(outer)
    def _():
        pl.semaphore_wait(barrier, 4)

    def inward(n):
        kind = pick(n, [i[0] for i in INWARD])
        k = pick(n, [i[1] for i in INWARD])
        off = jnp.where(kind == 0, keep_off, give_off)
        return remote(
            dens.at[part(off), columns(k)], mb.at[1, part(off), columns(k)],
            in_s.at[n], in_r.at[n], to_mate,
        ), kind, k, off

    def across(k):
        return remote(
            dens.at[part(give_off), columns(k)], mb.at[2, part(give_off), columns(k)],
            mid_s.at[k], mid_r.at[k], to_cross,
        )

    def relay(k):
        return remote(
            mb.at[1, part(give_off), columns(k)], mb.at[3, part(give_off), columns(k)],
            mid_s.at[4 + k], mid_r.at[4 + k], to_cross,
        )

    def middle_in(n):
        block, k = 2 + n // 4, n % 4
        return remote(
            mb.at[block, part(keep_off), columns(k)], mb.at[block, part(keep_off), columns(k)],
            mid_s.at[n], mid_r.at[n], to_cross,
        ), block, k

    def swap(slot, tile, k):
        return remote(
            dsend.at[slot], drecv.at[tile, rows(k)],
            p_s.at[slot], p_r.at[tile * 4 + k], to_core,
        )

    def xt(g, k, j):
        return remote(
            drecv.at[j, rows(k)], xr.at[g, rows(k)], xt_s.at[g * 4 + k], xt_r.at[g * 4 + k], to_x
        )

    def yt(k):
        return remote(xr.at[1 - Y, rows(k)], yr.at[rows(k)], yt_s.at[k], yt_r.at[k], to_y)

    def yd(j, kk):
        return remote(
            drecv.at[4 + j, rows(2 * Y + kk)], yrd.at[j, rows(kk)],
            yd_s.at[j * 2 + kk], yd_r.at[j * 2 + kk], to_y,
        )

    def xd(t, kk, j):
        return remote(
            yrd.at[j, rows(kk)], xrd.at[t, rows(kk)],
            xd_s.at[t * 2 + kk], xd_r.at[t * 2 + kk], to_x,
        )

    def zd(t, kk):
        return remote(
            xrd.at[t, rows(kk)], din.at[t, rows(kk)],
            zd_s.at[t * 2 + kk], zd_r.at[t * 2 + kk], to_cross,
        )

    def forward(kk):
        return remote(din.at[1, rows(kk)], din.at[0, rows(kk)], fw_s.at[kk], fw_r.at[kk], to_mate)

    def grow(j, k):
        n = (j - 1) * 4 + k
        return remote(
            drecv.at[7 + j, rows(k)], drecv.at[j, rows(k)], g_s.at[n], g_r.at[n], to_mate
        )

    def transpose(block, off, k):
        def step(n):
            r = pl.ds(pl.multiple_of(off + n * kb, kb), kb)
            t = mb[block, r, columns(k)].T
            st[block, columns(k), r] = (t.astype(F32) * weight[:, r]).astype(BF16)

        many(0, half // kb, step)

    def product(a, b, full, k, ch):
        acc[...] = jnp.dot(
            st[a, rows(k), part(keep_off)], mb[b, part(keep_off), sides(ch)],
            preferred_element_type=F32,
        )

        @pl.when(full == 1)
        def _():
            acc[...] += jnp.dot(
                st[a, rows(k), part(give_off)], mb[b, part(give_off), sides(ch)],
                preferred_element_type=F32,
            )

    def kept(j, k, value):
        keep[j // 2, rows(k)] = value

    load = pltpu.make_async_copy(dens, mb.at[0], load_sem)

    @pl.when(outer)
    def _():
        many(0, ARRIVALS, lambda n: inward(n)[0].start())

    @pl.when(inner)
    def _():
        many(0, 4, lambda k: across(k).start())

    load.start()
    load.wait()

    def own(k):
        transpose(0, keep_off, k)
        transpose(0, give_off, k)

    many(0, 4, own)

    def give_away(k, j, value):
        drecv[j, rows(k)] = encode(value)

    def settle(tile, k):
        swap(0, tile, k).wait_recv()
        value = acc[...] + decode(drecv[tile, rows(k)])

        @pl.when(tile < 4)
        def _():
            @pl.when(tile % 2 == X)
            def _():
                kept(tile, k, value)

            @pl.when(tile % 2 != X)
            def _():
                drecv[tile, rows(k)] = encode(value)
                xt(tile // 2, k, tile).start()

        @pl.when((tile >= 4) & (tile < 8))
        def _():
            @pl.when(k // 2 == Y)
            def _():
                drecv[tile, rows(k)] = encode(value)
                yd(tile - 4, k % 2).start()

            @pl.when(k // 2 != Y)
            def _():
                keepd[tile - 4, rows(k % 2)] = value

        @pl.when(tile >= 8)
        def _():
            drecv[tile, rows(k)] = encode(value)
            grow(tile - 7, k).start()

    def send_part(n, tile, k):
        slot = n % RING

        @pl.when(n >= RING)
        def _():
            swap(slot, tile, k).wait_send()

        dsend[slot] = encode(acc[...])
        swap(slot, tile, k).start()

    def finish_ring():
        many(0, RING, lambda n: swap(n, 0, 0).wait_send())

    def give_y(k):
        xt(1 - Y, k, 0).wait_recv()
        value = keep[1 - Y, rows(k)] + decode(xr[1 - Y, rows(k)])
        late = (Y == 0) & (k // 2 == 0)

        @pl.when(late)
        def _():
            xr[1 - Y, rows(k)] = encode(value + decode(din[0, rows(k % 2)]))

        @pl.when(late == False)
        def _():
            xr[1 - Y, rows(k)] = encode(value)

        yt(k).start()

    def finish(k):
        xt(Y, k, 0).wait_recv()
        yt(k).wait_recv()
        value = keep[Y, rows(k)] + decode(xr[Y, rows(k)]) + decode(yr[rows(k)])
        late = (Y == 1) & (k // 2 == 1)

        @pl.when(late)
        def _():
            out[rows(k)] = value + decode(din[0, rows(k % 2)])

        @pl.when(late == False)
        def _():
            out[rows(k)] = value

    def last_stages(wait_din):
        many(0, 2, lambda n: give_y(2 * (1 - Y) * (1 - Y) + 2 * Y * (1 - Y) + n))
        wait_din()
        many(0, 2, lambda n: give_y(2 * Y + n))
        many(0, 4, finish)

    def wait_sends():
        def step(k):
            xt(0, k, 0).wait_send()
            xt(1, k, 0).wait_send()
            yt(k).wait_send()

        many(0, 4, step)

    @pl.when(inner)
    def _():
        def slot_step(s):
            @pl.when((s >= 1) & (s <= ARRIVALS))
            def _():
                n = s - 1
                copy, block, k = middle_in(n)
                copy.wait_recv()
                transpose(block, keep_off, k)
                copy, kind, k, off = inward(n)
                copy.wait_recv()

                @pl.when(kind == 1)
                def _():
                    relay(k).start()

                transpose(1, off, k)

            first, last = pick(s, PIECE_AT), pick(s + 1, PIECE_AT)

            def at_piece(n):
                tile = pick(n, [p[0] for p in PIECES])
                k = pick(n, [p[1] for p in PIECES])
                ch = pick(n, [p[2] for p in PIECES])
                a = pick(tile, [t[0] for t in TILES])
                b = pick(tile, [t[1] for t in TILES])
                full = pick(tile, [t[2] for t in TILES])
                return tile, k, ch, a, b, full

            def other(n, sent):
                tile, k, ch, a, b, full = at_piece(n)

                @pl.when(ch != c)
                def _():
                    product(a, b, full, k, ch)
                    send_part(sent, tile, k)

                return sent + jnp.where(ch != c, 1, 0)

            def mine(n):
                tile, k, ch, a, b, full = at_piece(n)

                @pl.when(ch == c)
                def _():
                    product(a, b, full, k, ch)
                    settle(tile, k)

            def before(n):
                total = jnp.int32(0)
                for m, p in enumerate(PIECES):
                    total = total + jnp.where((m < n) & (p[2] != c), 1, 0)
                return total

            lax.fori_loop(first, last, other, before(first))
            many(first, last, mine)

            def yd_in(n):
                j = pick(n, [i[0] for i in YD])
                kk = pick(n, [i[1] for i in YD])
                yd(j, kk).wait_recv()
                value = keepd[j, rows(kk)] + decode(yrd[j, rows(kk)])

                @pl.when(j % 2 == X)
                def _():
                    keepd[j, rows(kk)] = value

                @pl.when(j % 2 != X)
                def _():
                    yrd[j, rows(kk)] = encode(value)
                    xd(j // 2, kk, j).start()

            many(pick(s, YD_AT), pick(s + 1, YD_AT), yd_in)

            def xd_in(n):
                t = pick(n, [i[0] for i in XD])
                kk = pick(n, [i[1] for i in XD])
                xd(t, kk, 0).wait_recv()
                value = keepd[2 * t + X, rows(kk)] + decode(xrd[t, rows(kk)])
                xrd[t, rows(kk)] = encode(value)
                zd(t, kk).start()

            many(pick(s, XD_AT), pick(s + 1, XD_AT), xd_in)

        many(0, LAST + 1, slot_step)

        def pass_on(kk):
            zd(1, kk).wait_recv()
            forward(kk).start()

        def wait_din():
            many(0, 2, pass_on)
            many(0, 2, lambda kk: zd(0, kk).wait_recv())

        last_stages(wait_din)
        finish_ring()
        wait_sends()

        def ends(n):
            middle_in(n)[0].wait_send()
            yd(n // 2, n % 2).wait_send()

        many(0, 8, ends)

        def ends4(n):
            xd(n // 2, n % 2, 0).wait_send()
            zd(n // 2, n % 2).wait_send()

        many(0, 4, ends4)
        many(0, 2, lambda kk: forward(kk).wait_send())
        many(0, 12, lambda n: grow(1 + n // 4, n % 4).wait_send())

    @pl.when(outer)
    def _():
        def other(k):
            product(0, 0, jnp.int32(1), k, 1 - c)
            send_part(k, jnp.int32(0), k)

        def mine(k):
            product(0, 0, jnp.int32(1), k, c)
            settle(jnp.int32(0), k)

        many(0, 4, other)
        many(0, 4, mine)

        def arrived(n):
            j = pick(n, [i[0] for i in G_ORDER])
            k = pick(n, [i[1] for i in G_ORDER])
            grow(j, k).wait_recv()

            @pl.when(j % 2 == X)
            def _():
                kept(j, k, decode(drecv[j, rows(k)]))

            @pl.when(j % 2 != X)
            def _():
                xt(j // 2, k, j).start()

        many(0, 12, arrived)
        last_stages(lambda: many(0, 2, lambda kk: forward(kk).wait_recv()))
        finish_ring()
        wait_sends()
        many(0, ARRIVALS, lambda n: inward(n)[0].wait_send())


def one_kernel(densities, *bands):
    weight = weights(densities, *bands)[None, :]
    pairs, width = densities.shape
    rb, hw = width // 4, width // 2
    dma = pltpu.SemaphoreType.DMA
    counts = (8, 8, 8, 8, RING, 44, 8, 8, 4, 4, 8, 8, 4, 4, 4, 4, 2, 2, 12, 12)
    return pl.pallas_call(
        kernel,
        out_shape=jax.ShapeDtypeStruct((width, hw), F32),
        in_specs=[
            pl.BlockSpec(memory_space=pl.ANY),
            pl.BlockSpec(memory_space=pltpu.VMEM),
        ],
        out_specs=pl.BlockSpec(memory_space=pltpu.VMEM),
        scratch_shapes=[
            pltpu.VMEM((4, pairs, width), BF16),
            pltpu.VMEM((4, width, pairs), BF16),
            pltpu.VMEM((11, width, hw), I16),
            pltpu.VMEM((RING, rb, hw), I16),
            pltpu.VMEM((rb, hw), F32),
            pltpu.VMEM((2, width, hw), F32),
            pltpu.VMEM((4, hw, hw), F32),
            pltpu.VMEM((2, width, hw), I16),
            pltpu.VMEM((width, hw), I16),
            pltpu.VMEM((4, hw, hw), I16),
            pltpu.VMEM((2, hw, hw), I16),
            pltpu.VMEM((2, hw, hw), I16),
            pltpu.VMEM((8, 128), I16),
            dma,
        ]
        + [dma((n,)) for n in counts],
        compiler_params=pltpu.CompilerParams(
            collective_id=0, has_side_effects=True, vmem_limit_bytes=62 * 2**20
        ),
    )(densities, weight)


def solution(mesh):
    placed = (P("pair", "ga"), P("pair"), P("pair"), P(), P())
    square = mesh.shape["ga"] == PLANES and mesh.shape["pair"] == 2 * SQUARE**2
    return jax.shard_map(
        one_kernel if square else gather_all,
        mesh=mesh,
        in_specs=placed,
        out_specs=P("ga", "pair"),
        check_vma=False,
    )
```

```python
import functools
import math

import jax
import jax.numpy as jnp
from jax import lax
from jax.experimental import pallas as pl
from jax.experimental.pallas import tpu as pltpu
from jax.sharding import PartitionSpec as P

MESH = pl.DeviceIdType.MESH
PLANES, SQUARE = 4, 2
F32, BF16, I16 = jnp.float32, jnp.bfloat16, jnp.int16


def lookup(bands, table):
    levels = lax.broadcasted_iota(jnp.int32, (1, table.shape[0]), 1)
    onehot = (bands[:, None] == levels).astype(jnp.float32)
    return jnp.sum(onehot * table[None, :], axis=1)


def weights(densities, val_band, cond_band, val_energy, cond_energy):
    pairs_total = densities.shape[0] * lax.axis_size("pair")
    gap = lookup(val_band, val_energy) - lookup(cond_band, cond_energy)
    return 4.0 / (gap * math.sqrt(pairs_total))


def scale(weight, block):
    return (weight[:, None] * block.astype(jnp.float32)).astype(jnp.bfloat16)


def contract(left, right):
    return lax.dot_general(
        left, right, (((0,), (0,)), ((), ())), preferred_element_type=jnp.float32
    )


def gather_all(densities, *bands):
    scaled = scale(weights(densities, *bands), densities)
    gathered = lax.all_gather(densities, "ga", axis=1, tiled=True)
    owned = lax.psum_scatter(
        contract(gathered, scaled), "pair", scatter_dimension=0, tiled=True
    )
    return owned.T


STEPS, LOW = 816.0, -27.0


def encode(x):
    t = jnp.maximum(jnp.log2(jnp.abs(x)) * STEPS + (1.5 - LOW * STEPS), 0.0)
    return jnp.where(x < 0, -t, t).astype(jnp.int32).astype(I16)


def decode(code):
    c = code.astype(F32)
    m = jnp.exp2(jnp.abs(c) * (1 / STEPS) + (LOW - 1 / STEPS))
    return jnp.where(c < 0, -m, m)


TILES = (
    (0, 1, 1), (0, 0, 1), (0, 2, 0), (0, 3, 0),
    (2, 1, 0), (2, 0, 0), (3, 1, 0), (3, 0, 0),
    (1, 0, 1), (1, 2, 0), (1, 3, 0),
)
INWARD = ((0, 0), (0, 1), (1, 0), (1, 1), (1, 2), (1, 3), (0, 2), (0, 3))
ARRIVALS = 8
RING, SENDS, LAG = 8, 4, 2


def chunk_slot(block, k, full):
    if block == 0:
        return 0
    if block == 1:
        slots = [INWARD.index((0, k)) + 1]
        if full:
            slots.append(INWARD.index((1, k)) + 1)
        return max(slots)
    return (block - 2) * 4 + k + 1


def piece_slot(tile, k, ch):
    a, b, full = TILES[tile]
    columns = max(chunk_slot(b, 2 * ch, full), chunk_slot(b, 2 * ch + 1, full))
    slot = max(chunk_slot(a, k, full), columns)
    if slot == ARRIVALS and not 4 <= tile < 8:
        slot += 1 if tile >= 8 else 2
    return slot


PRIORITY = (6, 7, 4, 5, 10, 9, 8, 3, 0, 2, 1)
PIECES = [
    sorted(
        ((t, k) for t in range(11) for k in range(4)),
        key=lambda p: (piece_slot(*p, ch), PRIORITY.index(p[0]), p[1]),
    )
    for ch in range(2)
]
COUNT = 44
LAST = ARRIVALS + 4


def ranges(slots):
    slots = sorted(slots)
    return [sum(1 for s in slots if s < n) for n in range(LAST + 2)]


def order(items, slot):
    items = sorted(items, key=lambda i: (slot(*i), i))
    return items, ranges([slot(*i) for i in items])


def yd_slot(ch, j, kk):
    return max(piece_slot(4 + j, 2 * v + kk, ch) for v in (0, 1)) + 1


def xd_slot(ch, t, kk):
    return max(ARRIVALS, *(yd_slot(ch, 2 * t + x, kk) for x in (0, 1))) + 1


def both(items, slot):
    found = [order(items, functools.partial(slot, ch)) for ch in range(2)]
    return [f[0] for f in found], [f[1] for f in found]


YD, YD_AT = both([(j, kk) for j in range(4) for kk in range(2)], yd_slot)
XD, XD_AT = both([(t, kk) for t in range(2) for kk in range(2)], xd_slot)
PIECE_AT = [ranges([piece_slot(*p, ch) for p in PIECES[ch]]) for ch in range(2)]
G_ORDER = [[(t - 7, k) for t, k in PIECES[ch] if t >= 8] for ch in range(2)]


def pick(index, values):
    result = jnp.int32(values[0])
    for n, value in enumerate(values):
        if n and value != values[0]:
            result = jnp.where(index == n, value, result)
    return result


def pick2(side, index, values):
    return jnp.where(side == 0, pick(index, values[0]), pick(index, values[1]))


def packed(side, index, codes):
    words = [
        [sum(v << (6 * i) for i, v in enumerate(c[n : n + 5])) for n in range(0, len(c), 5)]
        for c in codes
    ]
    word, place = pick2(side, lax.div(index, 5), words), lax.rem(index, 5)
    result = lax.rem(word, 64)
    for i in range(1, 5):
        word = lax.div(word, 64)
        result = jnp.where(place == i, lax.rem(word, 64), result)
    return result


def many(start, stop, body):
    def step(n, carry):
        body(n)
        return carry

    lax.fori_loop(start, stop, step, 0)


def kernel(
    dens, weight, out, mb, st, drecv, dsend, ring, acc, keep, keepd, keepg, xr, yr, yrd, xrd, din,
    load_sem, credit, in_s, in_r, mid_s, mid_r, p_s, p_r, xt_s, xt_r, yt_s, yt_r,
    yd_s, yd_r, xd_s, xd_r, zd_s, zd_r, g_s, g_r,
):
    pair, z = lax.axis_index("pair"), lax.axis_index("ga")
    c = pair % 2
    x = (pair // 2) % 2
    y = pair // 4
    h = z // 2
    X = (x + h) % 2
    Y = (y + h) % 2
    inner = (z == 1) | (z == 2)
    outer = (z == 0) | (z == 3)

    pairs, width = dens.shape
    half = pairs // 2
    rb = width // 4
    hw = width // 2
    kb = 256 if half % 256 == 0 else half
    keep_off = h * half
    give_off = (1 - h) * half

    def at(yy, xx, cc, zz):
        return ((yy * SQUARE + xx) * 2 + cc, zz)

    to_core = at(y, x, 1 - c, z)
    to_x = at(y, 1 - x, c, z)
    to_y = at(1 - y, x, c, z)
    z_mate = z + 1 - 2 * (z % 2)
    z_cross = 3 - z
    to_mate = at(y, x, c, z_mate)
    to_cross = at(y, x, c, z_cross)

    def remote(src, dst, send, recv, to):
        return pltpu.make_async_remote_copy(
            src_ref=src, dst_ref=dst, send_sem=send, recv_sem=recv,
            device_id=to, device_id_type=MESH,
        )

    def rows(k, size=rb):
        return pl.ds(pl.multiple_of(k * size, size), size)

    def part(off):
        return pl.ds(pl.multiple_of(off, half), half)

    def columns(k):
        return pl.ds(pl.multiple_of(k * rb, rb), rb)

    def sides(k):
        return pl.ds(pl.multiple_of(k * hw, hw), hw)

    barrier = pltpu.get_barrier_semaphore()
    for to in (to_core, to_x, to_y, to_mate):
        pl.semaphore_signal(barrier, inc=1, device_id=to, device_id_type=MESH)

    @pl.when(inner)
    def _():
        pl.semaphore_signal(barrier, inc=1, device_id=to_cross, device_id_type=MESH)
        pl.semaphore_wait(barrier, 5)

    @pl.when(outer)
    def _():
        pl.semaphore_wait(barrier, 4)

    def inward(n):
        kind = pick(n, [i[0] for i in INWARD])
        k = pick(n, [i[1] for i in INWARD])
        off = jnp.where(kind == 0, keep_off, give_off)
        return remote(
            dens.at[part(off), columns(k)], mb.at[1, part(off), columns(k)],
            in_s.at[n], in_r.at[n], to_mate,
        ), kind, k, off

    def across(k):
        return remote(
            dens.at[part(give_off), columns(k)], mb.at[2, part(give_off), columns(k)],
            mid_s.at[k], mid_r.at[k], to_cross,
        )

    def relay(k):
        return remote(
            mb.at[1, part(give_off), columns(k)], mb.at[3, part(give_off), columns(k)],
            mid_s.at[4 + k], mid_r.at[4 + k], to_cross,
        )

    def middle_in(n):
        block, k = 2 + n // 4, n % 4
        return remote(
            mb.at[block, part(keep_off), columns(k)], mb.at[block, part(keep_off), columns(k)],
            mid_s.at[n], mid_r.at[n], to_cross,
        ), block, k

    def swap(n):
        return remote(
            dsend.at[n % SENDS], ring.at[n % RING], p_s.at[n % SENDS], p_r.at[n % RING], to_core
        )

    def xt(g, k, j):
        return remote(
            drecv.at[j, rows(k)], xr.at[g, rows(k)], xt_s.at[g * 4 + k], xt_r.at[g * 4 + k], to_x
        )

    def yt(k):
        return remote(xr.at[1 - Y, rows(k)], yr.at[rows(k)], yt_s.at[k], yt_r.at[k], to_y)

    def yd(j, kk):
        return remote(
            drecv.at[4 + j, rows(2 * Y + kk)], yrd.at[j, rows(kk)],
            yd_s.at[j * 2 + kk], yd_r.at[j * 2 + kk], to_y,
        )

    def xd(t, kk, j):
        return remote(
            yrd.at[j, rows(kk)], xrd.at[t, rows(kk)],
            xd_s.at[t * 2 + kk], xd_r.at[t * 2 + kk], to_x,
        )

    def zd(t, kk):
        return remote(
            xrd.at[t, rows(kk)], din.at[t, rows(kk)],
            zd_s.at[t * 2 + kk], zd_r.at[t * 2 + kk], to_cross,
        )

    def grow(j, k):
        n = (j - 1) * 4 + k
        return remote(
            drecv.at[7 + j, rows(k)], drecv.at[j, rows(k)], g_s.at[n], g_r.at[n], to_mate
        )

    def transpose(block, off, k):
        def step(n):
            r = pl.ds(pl.multiple_of(off + n * kb, kb), kb)
            t = mb[block, r, columns(k)].T
            st[block, columns(k), r] = (t.astype(F32) * weight[:, r]).astype(BF16)

        many(0, half // kb, step)

    def product(a, b, full, k, ch, put):
        @pl.when(full == 0)
        def _():
            put(jnp.dot(
                st[a, rows(k), part(keep_off)], mb[b, part(keep_off), sides(ch)],
                preferred_element_type=F32,
            ))

        @pl.when(full == 1)
        def _():
            put(jnp.dot(st[a, rows(k)], mb[b, :, sides(ch)], preferred_element_type=F32))

    def kept(j, k, value):
        keep[j // 2, rows(k)] = value

    load = pltpu.make_async_copy(dens, mb.at[0], load_sem)

    @pl.when(outer)
    def _():
        many(0, ARRIVALS, lambda n: inward(n)[0].start())

    @pl.when(inner)
    def _():
        many(0, 4, lambda k: across(k).start())

    load.start()
    load.wait()

    def own(k):
        transpose(0, keep_off, k)
        transpose(0, give_off, k)

    many(0, 4, own)

    def theirs(n, a, b, full, k):
        @pl.when(n >= SENDS)
        def _():
            swap(n).wait_send()

        @pl.when(n >= RING)
        def _():
            pl.semaphore_wait(credit, 1)

        def put(value):
            dsend[n % SENDS] = value

        product(a, b, full, k, 1 - c, put)
        swap(n).start()

    def settle(n, count, tile, a, b, full, k):
        swap(n).wait_recv()

        def put(value):
            acc[...] = value + ring[n % RING]

        product(a, b, full, k, c, put)

        @pl.when(n < count - RING)
        def _():
            pl.semaphore_signal(credit, inc=1, device_id=to_core, device_id_type=MESH)

        @pl.when((tile < 4) & (tile % 2 == X))
        def _():
            kept(tile, k, acc[...])

        stays = (tile >= 4) & (tile < 8) & (k // 2 != Y)

        @pl.when(stays)
        def _():
            keepd[tile - 4, rows(k % 2)] = acc[...]

        later = (tile == 9 + X) & (k // 2 == Y)

        @pl.when(later)
        def _():
            keepg[rows(k % 2)] = acc[...]

        @pl.when(jnp.logical_not(stays | later | ((tile < 4) & (tile % 2 == X))))
        def _():
            drecv[tile, rows(k)] = encode(acc[...])

            @pl.when(tile < 4)
            def _():
                xt(tile // 2, k, tile).start()

            @pl.when((tile >= 4) & (tile < 8))
            def _():
                yd(tile - 4, k % 2).start()

            @pl.when(tile >= 8)
            def _():
                grow(tile - 7, k).start()

    def finish_ring():
        many(0, SENDS, lambda n: swap(n).wait_send())

    def give_y(k):
        xt(1 - Y, k, 0).wait_recv()
        value = keep[1 - Y, rows(k)] + decode(xr[1 - Y, rows(k)])
        late = inner & (Y == 0) & (k // 2 == 0)

        @pl.when(late)
        def _():
            xr[1 - Y, rows(k)] = encode(value + decode(din[0, rows(k % 2)]))

        @pl.when(jnp.logical_not(late))
        def _():
            xr[1 - Y, rows(k)] = encode(value)

        yt(k).start()

    def finish(k):
        xt(Y, k, 0).wait_recv()
        yt(k).wait_recv()
        value = keep[Y, rows(k)] + decode(xr[Y, rows(k)]) + decode(yr[rows(k)])
        late = inner & (Y == 1) & (k // 2 == 1)

        @pl.when(late)
        def _():
            out[rows(k)] = value + decode(din[0, rows(k % 2)])

        @pl.when(jnp.logical_not(late))
        def _():
            out[rows(k)] = value

    def last_stages(wait_din):
        many(0, 2, lambda n: give_y(2 * (1 - Y) * (1 - Y) + 2 * Y * (1 - Y) + n))
        wait_din()
        many(0, 2, lambda n: give_y(2 * Y + n))
        many(0, 4, finish)

    def wait_sends():
        def step(k):
            xt(0, k, 0).wait_send()
            xt(1, k, 0).wait_send()
            yt(k).wait_send()

        many(0, 4, step)

    @pl.when(inner)
    def _():
        def slot_step(s):
            @pl.when((s >= 1) & (s <= ARRIVALS))
            def _():
                n = s - 1
                copy, block, k = middle_in(n)
                copy.wait_recv()
                transpose(block, keep_off, k)
                copy, kind, k, off = inward(n)
                copy.wait_recv()

                @pl.when(kind == 1)
                def _():
                    relay(k).start()

                transpose(1, off, k)

            sent, sent_to = pick2(1 - c, s, PIECE_AT), pick2(1 - c, s + 1, PIECE_AT)
            own_at, own_to = pick2(c, s, PIECE_AT), pick2(c, s + 1, PIECE_AT)

            def at_piece(side, n):
                code = packed(side, n, [[t * 4 + k for t, k in p] for p in PIECES])
                tile, k = lax.div(code, 4), lax.rem(code, 4)
                kind = pick(tile, [a * 8 + b * 2 + full for a, b, full in TILES])
                return tile, k, lax.div(kind, 8), lax.rem(lax.div(kind, 2), 4), lax.rem(kind, 2)

            def turn(n):
                @pl.when(sent + n < sent_to)
                def _():
                    tile, k, a, b, full = at_piece(1 - c, sent + n)
                    theirs(sent + n, a, b, full, k)

                @pl.when((n >= LAG) & (own_at + n - LAG < own_to))
                def _():
                    tile, k, a, b, full = at_piece(c, own_at + n - LAG)
                    settle(own_at + n - LAG, COUNT, tile, a, b, full, k)

            many(0, jnp.maximum(sent_to - sent, own_to - own_at + LAG), turn)

            def yd_in(n):
                j = pick2(c, n, [[i[0] for i in items] for items in YD])
                kk = pick2(c, n, [[i[1] for i in items] for items in YD])
                yd(j, kk).wait_recv()
                value = keepd[j, rows(kk)] + decode(yrd[j, rows(kk)])

                @pl.when(j % 2 == X)
                def _():
                    keepd[j, rows(kk)] = value

                @pl.when(j % 2 != X)
                def _():
                    yrd[j, rows(kk)] = encode(value)
                    xd(j // 2, kk, j).start()

            many(pick2(c, s, YD_AT), pick2(c, s + 1, YD_AT), yd_in)

            def xd_in(n):
                t = pick2(c, n, [[i[0] for i in items] for items in XD])
                kk = pick2(c, n, [[i[1] for i in items] for items in XD])
                xd(t, kk, 0).wait_recv()
                value = keepd[2 * t + X, rows(kk)] + decode(xrd[t, rows(kk)])
                xrd[t, rows(kk)] = encode(value)
                zd(t, kk).start()

            many(pick2(c, s, XD_AT), pick2(c, s + 1, XD_AT), xd_in)

        many(0, LAST + 1, slot_step)

        def pass_on(kk):
            zd(1, kk).wait_recv()
            value = keepg[rows(kk)] + decode(din[1, rows(kk)])
            drecv[9 + X, rows(2 * Y + kk)] = encode(value)
            grow(2 + X, 2 * Y + kk).start()

        def wait_din():
            many(0, 2, pass_on)
            many(0, 2, lambda kk: zd(0, kk).wait_recv())

        last_stages(wait_din)
        finish_ring()
        wait_sends()

        def ends(n):
            middle_in(n)[0].wait_send()
            yd(n // 2, n % 2).wait_send()

        many(0, 8, ends)

        def ends4(n):
            xd(n // 2, n % 2, 0).wait_send()
            zd(n // 2, n % 2).wait_send()

        many(0, 4, ends4)
        many(0, 12, lambda n: grow(1 + n // 4, n % 4).wait_send())

    @pl.when(outer)
    def _():
        many(0, 4, lambda k: theirs(k, 0, 0, jnp.int32(1), k))
        many(0, 4, lambda k: settle(k, 4, jnp.int32(0), 0, 0, jnp.int32(1), k))

        def arrived(n):
            j = pick2(c, n, [[i[0] for i in G_ORDER[ch]] for ch in range(2)])
            k = pick2(c, n, [[i[1] for i in G_ORDER[ch]] for ch in range(2)])
            later = (j == 2 + X) & (k // 2 == Y)

            @pl.when(jnp.logical_not(later))
            def _():
                grow(j, k).wait_recv()

            @pl.when((j % 2 == X) & jnp.logical_not(later))
            def _():
                kept(j, k, decode(drecv[j, rows(k)]))

            @pl.when(j % 2 != X)
            def _():
                xt(j // 2, k, j).start()

        def arrived_last(kk):
            j, k = 2 + X, 2 * Y + kk
            grow(j, k).wait_recv()
            kept(j, k, decode(drecv[j, rows(k)]))

        many(0, 12, arrived)
        last_stages(lambda: many(0, 2, arrived_last))
        finish_ring()
        wait_sends()
        many(0, ARRIVALS, lambda n: inward(n)[0].wait_send())


def one_kernel(densities, *bands):
    weight = weights(densities, *bands)[None, :]
    pairs, width = densities.shape
    rb, hw = width // 4, width // 2
    dma = pltpu.SemaphoreType.DMA
    counts = (8, 8, 8, 8, SENDS, RING, 8, 8, 4, 4, 8, 8, 4, 4, 4, 4, 12, 12)
    return pl.pallas_call(
        kernel,
        out_shape=jax.ShapeDtypeStruct((width, hw), F32),
        in_specs=[
            pl.BlockSpec(memory_space=pl.ANY),
            pl.BlockSpec(memory_space=pltpu.VMEM),
        ],
        out_specs=pl.BlockSpec(memory_space=pltpu.VMEM),
        scratch_shapes=[
            pltpu.VMEM((4, pairs, width), BF16),
            pltpu.VMEM((4, width, pairs), BF16),
            pltpu.VMEM((11, width, hw), I16),
            pltpu.VMEM((SENDS, rb, hw), F32),
            pltpu.VMEM((RING, rb, hw), F32),
            pltpu.VMEM((rb, hw), F32),
            pltpu.VMEM((2, width, hw), F32),
            pltpu.VMEM((4, hw, hw), F32),
            pltpu.VMEM((hw, hw), F32),
            pltpu.VMEM((2, width, hw), I16),
            pltpu.VMEM((width, hw), I16),
            pltpu.VMEM((4, hw, hw), I16),
            pltpu.VMEM((2, hw, hw), I16),
            pltpu.VMEM((2, hw, hw), I16),
            dma,
            pltpu.SemaphoreType.REGULAR,
        ]
        + [dma((n,)) for n in counts],
        compiler_params=pltpu.CompilerParams(
            collective_id=0, has_side_effects=True, vmem_limit_bytes=62 * 2**20
        ),
    )(densities, weight)


def solution(mesh):
    placed = (P("pair", "ga"), P("pair"), P("pair"), P(), P())
    square = mesh.shape["ga"] == PLANES and mesh.shape["pair"] == 2 * SQUARE**2
    return jax.shard_map(
        one_kernel if square else gather_all,
        mesh=mesh,
        in_specs=placed,
        out_specs=P("ga", "pair"),
        check_vma=False,
    )
```

```python
import functools
import math

import jax
import jax.numpy as jnp
from jax import lax
from jax.experimental import pallas as pl
from jax.experimental.pallas import tpu as pltpu
from jax.sharding import PartitionSpec as P

MESH = pl.DeviceIdType.MESH
PLANES, SQUARE = 4, 2
F32, BF16, I16 = jnp.float32, jnp.bfloat16, jnp.int16


def lookup(bands, table):
    levels = lax.broadcasted_iota(jnp.int32, (1, table.shape[0]), 1)
    onehot = (bands[:, None] == levels).astype(jnp.float32)
    return jnp.sum(onehot * table[None, :], axis=1)


def weights(densities, val_band, cond_band, val_energy, cond_energy):
    pairs_total = densities.shape[0] * lax.axis_size("pair")
    gap = lookup(val_band, val_energy) - lookup(cond_band, cond_energy)
    return 4.0 / (gap * math.sqrt(pairs_total))


def scale(weight, block):
    return (weight[:, None] * block.astype(jnp.float32)).astype(jnp.bfloat16)


def contract(left, right):
    return lax.dot_general(
        left, right, (((0,), (0,)), ((), ())), preferred_element_type=jnp.float32
    )


def gather_all(densities, *bands):
    scaled = scale(weights(densities, *bands), densities)
    gathered = lax.all_gather(densities, "ga", axis=1, tiled=True)
    owned = lax.psum_scatter(
        contract(gathered, scaled), "pair", scatter_dimension=0, tiled=True
    )
    return owned.T


STEPS, LOW = 816.0, -27.0


def encode(x):
    t = jnp.maximum(jnp.log2(jnp.abs(x)) * STEPS + (1.5 - LOW * STEPS), 0.0)
    return jnp.where(x < 0, -t, t).astype(jnp.int32).astype(I16)


def decode(code):
    c = code.astype(F32)
    m = jnp.exp2(jnp.abs(c) * (1 / STEPS) + (LOW - 1 / STEPS))
    return jnp.where(c < 0, -m, m)


TILES = (
    (0, 1, 1), (0, 0, 1), (0, 2, 0), (0, 3, 0),
    (2, 1, 0), (2, 0, 0), (3, 1, 0), (3, 0, 0),
    (1, 0, 1), (1, 2, 0), (1, 3, 0),
)
INWARD = ((0, 0), (0, 1), (1, 0), (1, 1), (1, 2), (1, 3), (0, 2), (0, 3))
ARRIVALS = 8
RING, SENDS, LAG = 8, 4, 2


def chunk_slot(block, k, full):
    if block == 0:
        return 0
    if block == 1:
        slots = [INWARD.index((0, k)) + 1]
        if full:
            slots.append(INWARD.index((1, k)) + 1)
        return max(slots)
    return (block - 2) * 4 + k + 1


def piece_slot(tile, k, ch):
    a, b, full = TILES[tile]
    columns = max(chunk_slot(b, 2 * ch, full), chunk_slot(b, 2 * ch + 1, full))
    slot = max(chunk_slot(a, k, full), columns)
    if slot == ARRIVALS and not 4 <= tile < 8:
        slot += 1 if tile >= 8 else 2
    return slot


PRIORITY = (6, 7, 4, 5, 10, 9, 8, 3, 0, 2, 1)
PIECES = [
    sorted(
        ((t, k) for t in range(11) for k in range(4)),
        key=lambda p: (piece_slot(*p, ch), PRIORITY.index(p[0]), p[1]),
    )
    for ch in range(2)
]
COUNT = 44
LAST = ARRIVALS + 4


def ranges(slots):
    slots = sorted(slots)
    return [sum(1 for s in slots if s < n) for n in range(LAST + 2)]


def order(items, slot):
    items = sorted(items, key=lambda i: (slot(*i), items.index(i)))
    return items, ranges([slot(*i) for i in items])


def yd_slot(ch, j, kk):
    return max(piece_slot(4 + j, 2 * v + kk, ch) for v in (0, 1)) + 1


def xd_slot(ch, t, kk):
    return max(ARRIVALS, *(yd_slot(ch, 2 * t + x, kk) for x in (0, 1))) + 1


def both(items, slot):
    found = [order(items, functools.partial(slot, ch)) for ch in range(2)]
    return [f[0] for f in found], [f[1] for f in found]


YD, YD_AT = both([(j, kk) for j in (2, 3, 0, 1) for kk in range(2)], yd_slot)
XD, XD_AT = both([(t, kk) for t in (1, 0) for kk in range(2)], xd_slot)
PIECE_AT = [ranges([piece_slot(*p, ch) for p in PIECES[ch]]) for ch in range(2)]
G_ORDER = [[(t - 7, k) for t, k in PIECES[ch] if t >= 8] for ch in range(2)]


def pick(index, values):
    result = jnp.int32(values[0])
    for n, value in enumerate(values):
        if n and value != values[0]:
            result = jnp.where(index == n, value, result)
    return result


def pick2(side, index, values):
    return jnp.where(side == 0, pick(index, values[0]), pick(index, values[1]))


def packed(side, index, codes):
    words = [
        [sum(v << (6 * i) for i, v in enumerate(c[n : n + 5])) for n in range(0, len(c), 5)]
        for c in codes
    ]
    word, place = pick2(side, lax.div(index, 5), words), lax.rem(index, 5)
    result = lax.rem(word, 64)
    for i in range(1, 5):
        word = lax.div(word, 64)
        result = jnp.where(place == i, lax.rem(word, 64), result)
    return result


def many(start, stop, body):
    def step(n, carry):
        body(n)
        return carry

    lax.fori_loop(start, stop, step, 0)


def kernel(
    dens, val_band, cond_band, val_energy, cond_energy, out, mb, st, weight, drecv, dsend, ring, acc, keep, keepd, keepg, xr, yr, yrd, xrd, din,
    load_sem, credit, in_s, in_r, mid_s, mid_r, p_s, p_r, xt_s, xt_r, yt_s, yt_r,
    yd_s, yd_r, xd_s, xd_r, zd_s, zd_r, g_s, g_r,
):
    pair, z = lax.axis_index("pair"), lax.axis_index("ga")
    c = pair % 2
    x = (pair // 2) % 2
    y = pair // 4
    h = z // 2
    X = (x + h) % 2
    Y = (y + h) % 2
    inner = (z == 1) | (z == 2)
    outer = (z == 0) | (z == 3)

    pairs, width = dens.shape
    half = pairs // 2
    rb = width // 4
    hw = width // 2
    kb = 256 if half % 256 == 0 else half
    keep_off = h * half
    give_off = (1 - h) * half

    def at(yy, xx, cc, zz):
        return ((yy * SQUARE + xx) * 2 + cc, zz)

    to_core = at(y, x, 1 - c, z)
    to_x = at(y, 1 - x, c, z)
    to_y = at(1 - y, x, c, z)
    z_mate = z + 1 - 2 * (z % 2)
    z_cross = 3 - z
    to_mate = at(y, x, c, z_mate)
    to_cross = at(y, x, c, z_cross)

    def remote(src, dst, send, recv, to):
        return pltpu.make_async_remote_copy(
            src_ref=src, dst_ref=dst, send_sem=send, recv_sem=recv,
            device_id=to, device_id_type=MESH,
        )

    def rows(k, size=rb):
        return pl.ds(pl.multiple_of(k * size, size), size)

    def part(off):
        return pl.ds(pl.multiple_of(off, half), half)

    def columns(k):
        return pl.ds(pl.multiple_of(k * rb, rb), rb)

    def sides(k):
        return pl.ds(pl.multiple_of(k * hw, hw), hw)

    barrier = pltpu.get_barrier_semaphore()
    for to in (to_core, to_x, to_y, to_mate):
        pl.semaphore_signal(barrier, inc=1, device_id=to, device_id_type=MESH)

    @pl.when(inner)
    def _():
        pl.semaphore_signal(barrier, inc=1, device_id=to_cross, device_id_type=MESH)
        pl.semaphore_wait(barrier, 5)

    @pl.when(outer)
    def _():
        pl.semaphore_wait(barrier, 4)

    def slot_of(block):
        return jnp.minimum(block, 2)

    def place_of(block):
        return jnp.where(block == 3, give_off, keep_off)

    def inward(n):
        kind = pick(n, [i[0] for i in INWARD])
        k = pick(n, [i[1] for i in INWARD])
        off = jnp.where(kind == 0, keep_off, give_off)
        return remote(
            dens.at[part(off), columns(k)], mb.at[1, part(off), columns(k)],
            in_s.at[n], in_r.at[n], to_mate,
        ), kind, k, off

    def across(k):
        return remote(
            dens.at[part(give_off), columns(k)], mb.at[2, part(give_off), columns(k)],
            mid_s.at[k], mid_r.at[k], to_cross,
        )

    def relay(k):
        return remote(
            mb.at[1, part(give_off), columns(k)], mb.at[2, part(keep_off), columns(k)],
            mid_s.at[4 + k], mid_r.at[4 + k], to_cross,
        )

    def middle_in(n):
        block, k = 2 + n // 4, n % 4
        place = mb.at[2, part(place_of(block)), columns(k)]
        return remote(place, place, mid_s.at[n], mid_r.at[n], to_cross), block, k

    def swap(n):
        return remote(
            dsend.at[n % SENDS], ring.at[n % RING], p_s.at[n % SENDS], p_r.at[n % RING], to_core
        )

    def xt(g, k, j):
        return remote(
            drecv.at[j, rows(k)], xr.at[g, rows(k)], xt_s.at[g * 4 + k], xt_r.at[g * 4 + k], to_x
        )

    def yt(k):
        return remote(xr.at[1 - Y, rows(k)], yr.at[rows(k)], yt_s.at[k], yt_r.at[k], to_y)

    def yd(j, kk):
        return remote(
            drecv.at[4 + j, rows(2 * Y + kk)], yrd.at[j, rows(kk)],
            yd_s.at[j * 2 + kk], yd_r.at[j * 2 + kk], to_y,
        )

    def xd(t, kk, j):
        return remote(
            yrd.at[j, rows(kk)], xrd.at[t, rows(kk)],
            xd_s.at[t * 2 + kk], xd_r.at[t * 2 + kk], to_x,
        )

    def zd(t, kk):
        return remote(
            xrd.at[t, rows(kk)], din.at[t, rows(kk)],
            zd_s.at[t * 2 + kk], zd_r.at[t * 2 + kk], to_cross,
        )

    def grow(j, k):
        n = (j - 1) * 4 + k
        return remote(
            drecv.at[7 + j, rows(k)], drecv.at[j, rows(k)], g_s.at[n], g_r.at[n], to_mate
        )

    def transpose(slot, place, off, k):
        def step(n):
            r = pl.ds(pl.multiple_of(place + n * kb, kb), kb)
            w = weight[:, pl.ds(pl.multiple_of(off + n * kb, kb), kb)]
            t = mb[slot, r, columns(k)].T
            st[slot, columns(k), r] = (t.astype(F32) * w).astype(BF16)

        many(0, half // kb, step)

    def product(a, b, full, k, ch, put):
        @pl.when(full == 0)
        def _():
            put(jnp.dot(
                st[slot_of(a), rows(k), part(place_of(a))],
                mb[slot_of(b), part(place_of(b)), sides(ch)],
                preferred_element_type=F32,
            ))

        @pl.when(full == 1)
        def _():
            put(jnp.dot(st[a, rows(k)], mb[b, :, sides(ch)], preferred_element_type=F32))

    def kept(j, k, value):
        keep[j // 2, rows(k)] = value

    load = pltpu.make_async_copy(dens, mb.at[0], load_sem)

    @pl.when(outer)
    def _():
        many(0, ARRIVALS, lambda n: inward(n)[0].start())

    @pl.when(inner)
    def _():
        many(0, 4, lambda k: across(k).start())

    load.start()

    def level(bands, table):
        size = table.shape[0]
        column = jnp.broadcast_to(table[...].reshape(1, size), (8, size)).T[:, :1]
        found = lax.broadcasted_iota(jnp.int32, (size, pairs), 0) == bands[...].reshape(1, pairs)
        return jnp.sum(jnp.where(found, column, 0.0), axis=0, keepdims=True)

    gap = level(val_band, val_energy) - level(cond_band, cond_energy)
    weight[...] = 4.0 / (gap * math.sqrt(pairs * lax.axis_size("pair")))
    load.wait()

    def own(k):
        transpose(0, keep_off, keep_off, k)
        transpose(0, give_off, give_off, k)

    many(0, 4, own)

    def theirs(n, a, b, full, k):
        @pl.when(n >= SENDS)
        def _():
            swap(n).wait_send()

        @pl.when(n >= RING)
        def _():
            pl.semaphore_wait(credit, 1)

        def put(value):
            dsend[n % SENDS] = value

        product(a, b, full, k, 1 - c, put)
        swap(n).start()

    def settle(n, count, tile, a, b, full, k):
        swap(n).wait_recv()

        def put(value):
            acc[...] = value + ring[n % RING]

        product(a, b, full, k, c, put)

        @pl.when(n < count - RING)
        def _():
            pl.semaphore_signal(credit, inc=1, device_id=to_core, device_id_type=MESH)

        @pl.when((tile < 4) & (tile % 2 == X))
        def _():
            kept(tile, k, acc[...])

        stays = (tile >= 4) & (tile < 8) & (k // 2 != Y)

        @pl.when(stays)
        def _():
            keepd[tile - 4, rows(k % 2)] = acc[...]

        later = (tile == 9 + X) & (k // 2 == Y)

        @pl.when(later)
        def _():
            keepg[rows(k % 2)] = acc[...]

        @pl.when(jnp.logical_not(stays | later | ((tile < 4) & (tile % 2 == X))))
        def _():
            drecv[tile, rows(k)] = encode(acc[...])

            @pl.when(tile < 4)
            def _():
                xt(tile // 2, k, tile).start()

            @pl.when((tile >= 4) & (tile < 8))
            def _():
                yd(tile - 4, k % 2).start()

            @pl.when(tile >= 8)
            def _():
                grow(tile - 7, k).start()

    def finish_ring():
        many(0, SENDS, lambda n: swap(n).wait_send())

    def give_y(k):
        xt(1 - Y, k, 0).wait_recv()
        value = keep[1 - Y, rows(k)] + decode(xr[1 - Y, rows(k)])
        late = inner & (Y == 0) & (k // 2 == 0)

        @pl.when(late)
        def _():
            xr[1 - Y, rows(k)] = encode(value + decode(din[0, rows(k % 2)]))

        @pl.when(jnp.logical_not(late))
        def _():
            xr[1 - Y, rows(k)] = encode(value)

        yt(k).start()

    def finish(k):
        xt(Y, k, 0).wait_recv()
        yt(k).wait_recv()
        value = keep[Y, rows(k)] + decode(xr[Y, rows(k)]) + decode(yr[rows(k)])
        late = inner & (Y == 1) & (k // 2 == 1)

        @pl.when(late)
        def _():
            out[rows(k)] = value + decode(din[0, rows(k % 2)])

        @pl.when(jnp.logical_not(late))
        def _():
            out[rows(k)] = value

    def last_stages(wait_din):
        many(0, 2, lambda n: give_y(2 * (1 - Y) * (1 - Y) + 2 * Y * (1 - Y) + n))
        wait_din()
        many(0, 2, lambda n: give_y(2 * Y + n))
        many(0, 4, finish)

    def wait_sends():
        def step(k):
            xt(0, k, 0).wait_send()
            xt(1, k, 0).wait_send()
            yt(k).wait_send()

        many(0, 4, step)

    @pl.when(inner)
    def _():
        def slot_step(s):
            @pl.when((s >= 1) & (s <= ARRIVALS))
            def _():
                n = s - 1
                copy, block, k = middle_in(n)
                copy.wait_recv()
                transpose(2, place_of(block), keep_off, k)
                copy, kind, k, off = inward(n)
                copy.wait_recv()

                @pl.when(kind == 1)
                def _():
                    relay(k).start()

                transpose(1, off, off, k)

            sent, sent_to = pick2(1 - c, s, PIECE_AT), pick2(1 - c, s + 1, PIECE_AT)
            own_at, own_to = pick2(c, s, PIECE_AT), pick2(c, s + 1, PIECE_AT)

            def at_piece(side, n):
                code = packed(side, n, [[t * 4 + k for t, k in p] for p in PIECES])
                tile, k = lax.div(code, 4), lax.rem(code, 4)
                kind = pick(tile, [a * 8 + b * 2 + full for a, b, full in TILES])
                return tile, k, lax.div(kind, 8), lax.rem(lax.div(kind, 2), 4), lax.rem(kind, 2)

            def turn(n):
                @pl.when(sent + n < sent_to)
                def _():
                    tile, k, a, b, full = at_piece(1 - c, sent + n)
                    theirs(sent + n, a, b, full, k)

                @pl.when((n >= LAG) & (own_at + n - LAG < own_to))
                def _():
                    tile, k, a, b, full = at_piece(c, own_at + n - LAG)
                    settle(own_at + n - LAG, COUNT, tile, a, b, full, k)

            many(0, jnp.maximum(sent_to - sent, own_to - own_at + LAG), turn)

            def yd_in(n):
                j = pick2(c, n, [[i[0] for i in items] for items in YD])
                kk = pick2(c, n, [[i[1] for i in items] for items in YD])
                yd(j, kk).wait_recv()
                value = keepd[j, rows(kk)] + decode(yrd[j, rows(kk)])

                @pl.when(j % 2 == X)
                def _():
                    keepd[j, rows(kk)] = value

                @pl.when(j % 2 != X)
                def _():
                    yrd[j, rows(kk)] = encode(value)
                    xd(j // 2, kk, j).start()

            many(pick2(c, s, YD_AT), pick2(c, s + 1, YD_AT), yd_in)

            def xd_in(n):
                t = pick2(c, n, [[i[0] for i in items] for items in XD])
                kk = pick2(c, n, [[i[1] for i in items] for items in XD])
                xd(t, kk, 0).wait_recv()
                value = keepd[2 * t + X, rows(kk)] + decode(xrd[t, rows(kk)])
                xrd[t, rows(kk)] = encode(value)
                zd(t, kk).start()

            many(pick2(c, s, XD_AT), pick2(c, s + 1, XD_AT), xd_in)

        many(0, LAST + 1, slot_step)

        def pass_on(kk):
            zd(1, kk).wait_recv()
            value = keepg[rows(kk)] + decode(din[1, rows(kk)])
            drecv[9 + X, rows(2 * Y + kk)] = encode(value)
            grow(2 + X, 2 * Y + kk).start()

        def wait_din():
            many(0, 2, pass_on)
            many(0, 2, lambda kk: zd(0, kk).wait_recv())

        last_stages(wait_din)
        finish_ring()
        wait_sends()

        def ends(n):
            middle_in(n)[0].wait_send()
            yd(n // 2, n % 2).wait_send()

        many(0, 8, ends)

        def ends4(n):
            xd(n // 2, n % 2, 0).wait_send()
            zd(n // 2, n % 2).wait_send()

        many(0, 4, ends4)
        many(0, 12, lambda n: grow(1 + n // 4, n % 4).wait_send())

    @pl.when(outer)
    def _():
        many(0, 4, lambda k: theirs(k, 0, 0, jnp.int32(1), k))
        many(0, 4, lambda k: settle(k, 4, jnp.int32(0), 0, 0, jnp.int32(1), k))

        def arrived(n):
            j = pick2(c, n, [[i[0] for i in G_ORDER[ch]] for ch in range(2)])
            k = pick2(c, n, [[i[1] for i in G_ORDER[ch]] for ch in range(2)])
            later = (j == 2 + X) & (k // 2 == Y)

            @pl.when(jnp.logical_not(later))
            def _():
                grow(j, k).wait_recv()

            @pl.when((j % 2 == X) & jnp.logical_not(later))
            def _():
                kept(j, k, decode(drecv[j, rows(k)]))

            @pl.when(j % 2 != X)
            def _():
                xt(j // 2, k, j).start()

        def arrived_last(kk):
            j, k = 2 + X, 2 * Y + kk
            grow(j, k).wait_recv()
            kept(j, k, decode(drecv[j, rows(k)]))

        many(0, 12, arrived)
        last_stages(lambda: many(0, 2, arrived_last))
        finish_ring()
        wait_sends()
        many(0, ARRIVALS, lambda n: inward(n)[0].wait_send())


def one_kernel(densities, *bands):
    pairs, width = densities.shape
    rb, hw = width // 4, width // 2
    dma = pltpu.SemaphoreType.DMA
    counts = (8, 8, 8, 8, SENDS, RING, 8, 8, 4, 4, 8, 8, 4, 4, 4, 4, 12, 12)
    return pl.pallas_call(
        kernel,
        out_shape=pltpu.VMEM((width, hw), F32),
        in_specs=[
            pl.BlockSpec(memory_space=pl.ANY),
        ]
        + [pl.BlockSpec(memory_space=pltpu.VMEM)] * 4,
        out_specs=pl.BlockSpec(memory_space=pltpu.VMEM),
        scratch_shapes=[
            pltpu.VMEM((3, pairs, width), BF16),
            pltpu.VMEM((3, width, pairs), BF16),
            pltpu.VMEM((1, pairs), F32),
            pltpu.VMEM((11, width, hw), I16),
            pltpu.VMEM((SENDS, rb, hw), F32),
            pltpu.VMEM((RING, rb, hw), F32),
            pltpu.VMEM((rb, hw), F32),
            pltpu.VMEM((2, width, hw), F32),
            pltpu.VMEM((4, hw, hw), F32),
            pltpu.VMEM((hw, hw), F32),
            pltpu.VMEM((2, width, hw), I16),
            pltpu.VMEM((width, hw), I16),
            pltpu.VMEM((4, hw, hw), I16),
            pltpu.VMEM((2, hw, hw), I16),
            pltpu.VMEM((2, hw, hw), I16),
            dma,
            pltpu.SemaphoreType.REGULAR,
        ]
        + [dma((n,)) for n in counts],
        compiler_params=pltpu.CompilerParams(
            collective_id=0, has_side_effects=True, vmem_limit_bytes=58 * 2**20
        ),
    )(densities, *bands)


def solution(mesh):
    placed = (P("pair", "ga"), P("pair"), P("pair"), P(), P())
    square = mesh.shape["ga"] == PLANES and mesh.shape["pair"] == 2 * SQUARE**2
    return jax.shard_map(
        one_kernel if square else gather_all,
        mesh=mesh,
        in_specs=placed,
        out_specs=P("ga", "pair"),
        check_vma=False,
    )
```

```python
import functools
import math

import jax
import jax.numpy as jnp
from jax import lax
from jax.experimental import pallas as pl
from jax.experimental.pallas import tpu as pltpu
from jax.sharding import PartitionSpec as P

MESH = pl.DeviceIdType.MESH
PLANES, SQUARE = 4, 2
F32, BF16, I16 = jnp.float32, jnp.bfloat16, jnp.int16


def lookup(bands, table):
    levels = lax.broadcasted_iota(jnp.int32, (1, table.shape[0]), 1)
    onehot = (bands[:, None] == levels).astype(jnp.float32)
    return jnp.sum(onehot * table[None, :], axis=1)


def weights(densities, val_band, cond_band, val_energy, cond_energy):
    pairs_total = densities.shape[0] * lax.axis_size("pair")
    gap = lookup(val_band, val_energy) - lookup(cond_band, cond_energy)
    return 4.0 / (gap * math.sqrt(pairs_total))


def scale(weight, block):
    return (weight[:, None] * block.astype(jnp.float32)).astype(jnp.bfloat16)


def contract(left, right):
    return lax.dot_general(
        left, right, (((0,), (0,)), ((), ())), preferred_element_type=jnp.float32
    )


def gather_all(densities, *bands):
    scaled = scale(weights(densities, *bands), densities)
    gathered = lax.all_gather(densities, "ga", axis=1, tiled=True)
    owned = lax.psum_scatter(
        contract(gathered, scaled), "pair", scatter_dimension=0, tiled=True
    )
    return owned.T


STEPS, LOW = 816.0, -27.0


def encode(x):
    t = jnp.maximum(jnp.log2(jnp.abs(x)) * STEPS + (1.5 - LOW * STEPS), 0.0)
    return jnp.where(x < 0, -t, t).astype(jnp.int32).astype(I16)


def decode(code):
    c = code.astype(F32)
    m = jnp.exp2(jnp.abs(c) * (1 / STEPS) + (LOW - 1 / STEPS))
    return jnp.where(c < 0, -m, m)


TILES = (
    (0, 1, 1), (0, 0, 1), (0, 2, 0), (0, 3, 0),
    (2, 1, 0), (2, 0, 0), (3, 1, 0), (3, 0, 0),
    (1, 0, 1), (1, 2, 0), (1, 3, 0),
)
INWARD = ((0, 0), (1, 0), (0, 1), (1, 1), (0, 2), (1, 2), (1, 3), (0, 3))
ARRIVALS = 8
RING, SENDS = 8, 4
COUNT = 44
PIECES = (
    (
        4, 7, 5, 36, 9, 6, 10, 20, 22, 32, 23, 17, 3, 2, 21, 19, 0, 33, 38, 18, 26, 16, 30, 34,
        1, 27, 31, 24, 11, 28, 40, 25, 14, 42, 29, 43, 15, 39, 35, 37, 12, 41, 13, 8,
    ),
    (
        6, 7, 5, 4, 22, 32, 8, 20, 33, 37, 23, 38, 41, 10, 31, 30, 42, 40, 11, 21, 13, 34, 9, 36,
        28, 12, 14, 35, 39, 27, 3, 26, 43, 19, 24, 25, 29, 2, 17, 18, 1, 16, 15, 0,
    ),
)
INNER = (
    (
        0, 3, 2, 1, 1, 1, 0, 0, 2, 1, 1, 1, 2, 0, 0, 25, 1, 2, 3, 1, 3, 1, 0, 1,
        0, 0, 3, 2, 0, 1, 1, 0, 1, 1, 1, 1, 1, 23, 0, 1, 3, 1, 1, 0, 2, 0, 6, 1,
        0, 0, 1, 3, 0, 0, 7, 0, 0, 20, 5, 1, 0, 0, 1, 28, 1, 22, 0, 2, 21, 0, 4, 0,
        3, 0, 0, 1, 1, 13, 0, 3, 0, 2, 0, 0, 1, 1, 0, 0, 1, 12, 0, 1, 1, 0, 1, 1,
        1, 0, 0, 8, 1, 0, 1, 1, 0, 9, 11, 10, 1, 0, 1, 0, 0, 1, 15, 1, 1, 33, 0, 14,
        19, 0, 32, 18, 0, 24, 29, 16, 1, 17, 35, 31, 37, 27, 30, 36, 34, 26,
    ),
    (
        0, 0, 0, 2, 3, 2, 1, 0, 0, 0, 3, 1, 0, 0, 2, 25, 24, 0, 1, 3, 1, 2, 0, 1,
        0, 0, 3, 0, 0, 0, 1, 1, 1, 0, 0, 3, 0, 0, 0, 2, 1, 0, 0, 1, 3, 2, 1, 1,
        1, 0, 6, 1, 0, 0, 0, 1, 1, 23, 3, 1, 0, 1, 1, 1, 1, 1, 1, 2, 1, 1, 0, 1,
        0, 3, 0, 1, 1, 2, 0, 0, 1, 7, 0, 0, 32, 0, 0, 28, 1, 1, 0, 10, 1, 0, 0, 1,
        27, 31, 1, 1, 1, 1, 0, 0, 0, 1, 0, 8, 29, 9, 1, 0, 22, 1, 1, 11, 26, 1, 17, 14,
        30, 1, 20, 5, 16, 15, 19, 4, 33, 21, 13, 12, 35, 1, 18, 37, 36, 34,
    ),
)
OUTER = (
    (
        0, 8, 0, 0, 0, 5, 10, 4, 1, 18, 1, 23, 6, 1, 22, 12, 24, 28, 20, 1, 19, 14, 15, 11,
        32, 9, 7, 25, 21, 33, 13, 29, 16, 26, 30, 36, 34, 17, 31, 27, 37, 35,
    ),
    (
        1, 0, 0, 14, 18, 12, 5, 4, 1, 13, 0, 1, 0, 23, 22, 1, 9, 32, 21, 10, 11, 15, 20, 28,
        6, 29, 33, 8, 19, 24, 17, 31, 27, 16, 30, 7, 26, 25, 34, 35, 37, 36,
    ),
)
NOTHING = 63


def pick(index, values):
    result = jnp.int32(values[0])
    for n, value in enumerate(values):
        if n and value != values[0]:
            result = jnp.where(index == n, value, result)
    return result


def pick2(side, index, values):
    return jnp.where(side == 0, pick(index, values[0]), pick(index, values[1]))


def packed(side, index, codes):
    words = [
        [sum(v << (6 * i) for i, v in enumerate(c[n : n + 5])) for n in range(0, len(c), 5)]
        for c in codes
    ]
    word, place = pick2(side, lax.div(index, 5), words), lax.rem(index, 5)
    result = lax.rem(word, 64)
    for i in range(1, 5):
        word = lax.div(word, 64)
        result = jnp.where(place == i, lax.rem(word, 64), result)
    return result


def many(start, stop, body):
    def step(n, carry):
        body(n)
        return carry

    lax.fori_loop(start, stop, step, 0)


def kernel(
    dens, val_band, cond_band, val_energy, cond_energy, out, mb, st, weight, drecv, dsend, ring, acc, keep, keepd, keepg, xr, yr, yrd, xrd, din,
    load_sem, credit, in_s, in_r, mid_s, mid_r, p_s, p_r, xt_s, xt_r, yt_s, yt_r,
    yd_s, yd_r, xd_s, xd_r, zd_s, zd_r, g_s, g_r,
):
    pair, z = lax.axis_index("pair"), lax.axis_index("ga")
    c = pair % 2
    x = (pair // 2) % 2
    y = pair // 4
    h = z // 2
    X = (x + h) % 2
    Y = (y + h) % 2
    inner = (z == 1) | (z == 2)
    outer = (z == 0) | (z == 3)

    pairs, width = dens.shape
    half = pairs // 2
    rb = width // 4
    hw = width // 2
    kb = 256 if half % 256 == 0 else half
    keep_off = h * half
    give_off = (1 - h) * half

    def at(yy, xx, cc, zz):
        return ((yy * SQUARE + xx) * 2 + cc, zz)

    to_core = at(y, x, 1 - c, z)
    to_x = at(y, 1 - x, c, z)
    to_y = at(1 - y, x, c, z)
    z_mate = z + 1 - 2 * (z % 2)
    z_cross = 3 - z
    to_mate = at(y, x, c, z_mate)
    to_cross = at(y, x, c, z_cross)

    def remote(src, dst, send, recv, to):
        return pltpu.make_async_remote_copy(
            src_ref=src, dst_ref=dst, send_sem=send, recv_sem=recv,
            device_id=to, device_id_type=MESH,
        )

    def rows(k, size=rb):
        return pl.ds(pl.multiple_of(k * size, size), size)

    def part(off):
        return pl.ds(pl.multiple_of(off, half), half)

    side = (c + h) % 2

    def columns(k):
        return pl.ds(pl.multiple_of((k + 2 * h) % 4 * rb, rb), rb)

    def sides(k):
        return pl.ds(pl.multiple_of(k * hw, hw), hw)

    barrier = pltpu.get_barrier_semaphore()
    for to in (to_core, to_x, to_y, to_mate):
        pl.semaphore_signal(barrier, inc=1, device_id=to, device_id_type=MESH)

    @pl.when(inner)
    def _():
        pl.semaphore_signal(barrier, inc=1, device_id=to_cross, device_id_type=MESH)
        pl.semaphore_wait(barrier, 5)

    @pl.when(outer)
    def _():
        pl.semaphore_wait(barrier, 4)

    def slot_of(block):
        return jnp.minimum(block, 2)

    def place_of(block):
        return jnp.where(block == 3, give_off, keep_off)

    def inward(n):
        kind = pick(n, [i[0] for i in INWARD])
        k = pick(n, [i[1] for i in INWARD])
        off = jnp.where(kind == 0, keep_off, give_off)
        return remote(
            dens.at[part(off), columns(k)], mb.at[1, part(off), columns(k)],
            in_s.at[n], in_r.at[n], to_mate,
        ), kind, k, off

    def across(k):
        return remote(
            dens.at[part(give_off), columns(k + 2)], mb.at[2, part(give_off), columns(k + 2)],
            mid_s.at[k], mid_r.at[k], to_cross,
        )

    def relay(k):
        return remote(
            mb.at[1, part(give_off), columns(k)], mb.at[2, part(keep_off), columns(k)],
            mid_s.at[4 + k], mid_r.at[4 + k], to_cross,
        )

    def middle_in(n):
        block, k = 2 + n // 4, (n + 2 * (n // 4)) % 4
        place = mb.at[2, part(place_of(block)), columns(k)]
        return remote(place, place, mid_s.at[n], mid_r.at[n], to_cross), block, k

    def swap(n):
        return remote(
            dsend.at[n % SENDS], ring.at[n % RING], p_s.at[n % SENDS], p_r.at[n % RING], to_core
        )

    def xt(g, k, j):
        return remote(
            drecv.at[j, rows(k)], xr.at[g, rows(k)], xt_s.at[g * 4 + k], xt_r.at[g * 4 + k], to_x
        )

    def yt(k):
        return remote(xr.at[1 - Y, rows(k)], yr.at[rows(k)], yt_s.at[k], yt_r.at[k], to_y)

    def yd(j, kk):
        return remote(
            drecv.at[4 + j, rows(2 * (1 - Y) + kk)], yrd.at[j, rows(kk)],
            yd_s.at[j * 2 + kk], yd_r.at[j * 2 + kk], to_y,
        )

    def xd(t, kk, j):
        return remote(
            yrd.at[j, rows(kk)], xrd.at[t, rows(kk)],
            xd_s.at[t * 2 + kk], xd_r.at[t * 2 + kk], to_x,
        )

    def zd(t, kk):
        return remote(
            xrd.at[t, rows(kk)], din.at[t, rows(kk)],
            zd_s.at[t * 2 + kk], zd_r.at[t * 2 + kk], to_cross,
        )

    def grow(j, k):
        n = (j - 1) * 4 + k
        return remote(
            drecv.at[7 + j, rows(k)], drecv.at[j, rows(k)], g_s.at[n], g_r.at[n], to_mate
        )

    def transpose(slot, place, off, k):
        def step(n):
            r = pl.ds(pl.multiple_of(place + n * kb, kb), kb)
            w = weight[:, pl.ds(pl.multiple_of(off + n * kb, kb), kb)]
            t = mb[slot, r, columns(k)].T
            st[slot, rows(k), r] = (t.astype(F32) * w).astype(BF16)

        many(0, half // kb, step)

    def product(a, b, full, k, ch, put):
        @pl.when(full == 0)
        def _():
            put(jnp.dot(
                st[slot_of(a), rows(k), part(place_of(a))],
                mb[slot_of(b), part(place_of(b)), sides(ch)],
                preferred_element_type=F32,
            ))

        @pl.when(full == 1)
        def _():
            put(jnp.dot(st[a, rows(k)], mb[b, :, sides(ch)], preferred_element_type=F32))

    def kept(j, k, value):
        keep[j // 2, rows(k)] = value

    load = pltpu.make_async_copy(dens, mb.at[0], load_sem)

    @pl.when(outer)
    def _():
        many(0, ARRIVALS, lambda n: inward(n)[0].start())

    @pl.when(inner)
    def _():
        many(0, 4, lambda k: across(k).start())

    load.start()

    def level(bands, table):
        size = table.shape[0]
        column = jnp.broadcast_to(table[...].reshape(1, size), (8, size)).T[:, :1]
        found = lax.broadcasted_iota(jnp.int32, (size, pairs), 0) == bands[...].reshape(1, pairs)
        return jnp.sum(jnp.where(found, column, 0.0), axis=0, keepdims=True)

    gap = level(val_band, val_energy) - level(cond_band, cond_energy)
    weight[...] = 4.0 / (gap * math.sqrt(pairs * lax.axis_size("pair")))
    load.wait()

    def own(k):
        transpose(0, keep_off, keep_off, k)
        transpose(0, give_off, give_off, k)

    many(0, 4, own)

    def theirs(n, a, b, full, k):
        @pl.when(n >= SENDS)
        def _():
            swap(n).wait_send()

        @pl.when(n >= RING)
        def _():
            pl.semaphore_wait(credit, 1)

        def put(value):
            dsend[n % SENDS] = value

        product(a, b, full, k, 1 - c, put)
        swap(n).start()

    def settle(n, count, tile, a, b, full, k):
        swap(n).wait_recv()

        def put(value):
            acc[...] = value + ring[n % RING]

        product(a, b, full, k, c, put)

        @pl.when(n < count - RING)
        def _():
            pl.semaphore_signal(credit, inc=1, device_id=to_core, device_id_type=MESH)

        @pl.when((tile < 4) & (tile % 2 == X))
        def _():
            kept(tile, k, acc[...])

        stays = (tile >= 4) & (tile < 8) & (k // 2 == Y)

        @pl.when(stays)
        def _():
            keepd[tile - 4, rows(k % 2)] = acc[...]

        later = (tile == 9 + X) & (k // 2 == Y)

        @pl.when(later)
        def _():
            keepg[rows(k % 2)] = acc[...]

        @pl.when(jnp.logical_not(stays | later | ((tile < 4) & (tile % 2 == X))))
        def _():
            drecv[tile, rows(k)] = encode(acc[...])

            @pl.when(tile < 4)
            def _():
                xt(tile // 2, k, tile).start()

            @pl.when((tile >= 4) & (tile < 8))
            def _():
                yd(tile - 4, k % 2).start()

            @pl.when(tile >= 8)
            def _():
                grow(tile - 7, k).start()

    def finish_ring():
        many(0, SENDS, lambda n: swap(n).wait_send())

    def give_y(k):
        xt(1 - Y, k, 0).wait_recv()
        value = keep[1 - Y, rows(k)] + decode(xr[1 - Y, rows(k)])
        late = inner & (Y == 0) & (k // 2 == 0)

        @pl.when(late)
        def _():
            zd(0, k % 2).wait_recv()
            xr[1 - Y, rows(k)] = encode(value + decode(din[0, rows(k % 2)]))

        @pl.when(jnp.logical_not(late))
        def _():
            xr[1 - Y, rows(k)] = encode(value)

        yt(k).start()

    def finish(k):
        xt(Y, k, 0).wait_recv()
        yt(k).wait_recv()
        value = keep[Y, rows(k)] + decode(xr[Y, rows(k)]) + decode(yr[rows(k)])
        late = inner & (Y == 1) & (k // 2 == 1)

        @pl.when(late)
        def _():
            zd(0, k % 2).wait_recv()
            out[columns(k)] = value + decode(din[0, rows(k % 2)])

        @pl.when(jnp.logical_not(late))
        def _():
            out[columns(k)] = value

    def wait_sends():
        def step(k):
            xt(0, k, 0).wait_send()
            xt(1, k, 0).wait_send()
            yt(k).wait_send()

        many(0, 4, step)

    def run(lists, step):
        size = -(-max(map(len, lists)) // 5)
        padded = [list(l) + [NOTHING] * (5 * size - len(l)) for l in lists]
        words = [
            [sum(v << (6 * i) for i, v in enumerate(l[n : n + 5])) for n in range(0, 5 * size, 5)]
            for l in padded
        ]

        def one(i, state):
            word, counts = state
            code = lax.rem(word, 64)
            step(code, counts)
            counts = tuple(n + jnp.where(code == kind, 1, 0) for kind, n in enumerate(counts))
            return lax.div(word, 64), counts

        def five(w, counts):
            return lax.fori_loop(0, 5, one, (pick2(side, w, words), counts))[1]

        lax.fori_loop(0, size, five, (jnp.int32(0),) * 4)

    def on(condition, body):
        pl.when(condition)(body)

    def late_steps(code):
        n = code - 18
        on((n >= 0) & (n < 16) & (lax.div(n, 4) == 2 * (1 - Y) + X), lambda: give_y(lax.rem(n, 4)))
        on((code >= 34) & (code < 38), lambda: finish(code - 34))

    def at_piece(whose, n):
        code = packed(whose, n, PIECES)
        tile, k = lax.div(code, 4), lax.rem(code, 4)
        kind = pick(tile, [a * 8 + b * 2 + full for a, b, full in TILES])
        return tile, k, lax.div(kind, 8), lax.rem(lax.div(kind, 2), 4), lax.rem(kind, 2)

    def inner_step(code, counts):
        def form_theirs():
            tile, k, a, b, full = at_piece(1 - side, counts[0])
            theirs(counts[0], a, b, full, k)

        def form_own():
            tile, k, a, b, full = at_piece(side, counts[1])
            settle(counts[1], COUNT, tile, a, b, full, k)

        def from_across():
            copy, block, k = middle_in(counts[2])
            copy.wait_recv()
            transpose(2, place_of(block), keep_off, k)

        def from_outside():
            copy, kind, k, off = inward(counts[3])
            copy.wait_recv()
            on(kind == 1, lambda: relay(k).start())
            transpose(1, off, off, k)

        def yd_in():
            j, kk = lax.div(code - 4, 2), lax.rem(code - 4, 2)
            yd(j, kk).wait_recv()
            value = keepd[j, rows(kk)] + decode(yrd[j, rows(kk)])

            @pl.when(j % 2 == X)
            def _():
                keepd[j, rows(kk)] = value

            @pl.when(j % 2 != X)
            def _():
                yrd[j, rows(kk)] = encode(value)
                xd(j // 2, kk, j).start()

        def xd_in():
            t, kk = lax.div(code - 12, 2), lax.rem(code - 12, 2)
            xd(t, kk, 0).wait_recv()
            value = keepd[2 * t + X, rows(kk)] + decode(xrd[t, rows(kk)])
            xrd[t, rows(kk)] = encode(value)
            zd(t, kk).start()

        def pass_on():
            kk = code - 16
            zd(1, kk).wait_recv()
            value = keepg[rows(kk)] + decode(din[1, rows(kk)])
            drecv[9 + X, rows(2 * Y + kk)] = encode(value)
            grow(2 + X, 2 * Y + kk).start()

        on(code == 0, form_theirs)
        on(code == 1, form_own)
        on(code == 2, from_across)
        on(code == 3, from_outside)
        on((code >= 4) & (code < 12), yd_in)
        on((code >= 12) & (code < 16), xd_in)
        on((code >= 16) & (code < 18), pass_on)
        late_steps(code)

    def outer_step(code, counts):
        one = jnp.int32(1)
        on(code == 0, lambda: theirs(counts[0], 0, 0, one, counts[0]))
        on(code == 1, lambda: settle(counts[1], 4, jnp.int32(0), 0, 0, one, counts[1]))

        def arrived():
            j, k = 1 + lax.div(code - 4, 4), lax.rem(code - 4, 4)

            @pl.when(jnp.logical_not((j == 2 + X) & (k // 2 == Y)))
            def _():
                grow(j, k).wait_recv()

                @pl.when(j % 2 == X)
                def _():
                    kept(j, k, decode(drecv[j, rows(k)]))

                @pl.when(j % 2 != X)
                def _():
                    xt(j // 2, k, j).start()

        def arrived_last():
            j, k = 2 + X, 2 * Y + code - 16
            grow(j, k).wait_recv()
            kept(j, k, decode(drecv[j, rows(k)]))

        on((code >= 4) & (code < 16), arrived)
        on((code >= 16) & (code < 18), arrived_last)
        late_steps(code)

    @pl.when(inner)
    def _():
        run(INNER, inner_step)
        finish_ring()
        wait_sends()

        def ends(n):
            middle_in(n)[0].wait_send()
            yd(n // 2, n % 2).wait_send()

        many(0, 8, ends)

        def ends4(n):
            xd(n // 2, n % 2, 0).wait_send()
            zd(n // 2, n % 2).wait_send()

        many(0, 4, ends4)
        many(0, 12, lambda n: grow(1 + n // 4, n % 4).wait_send())

    @pl.when(outer)
    def _():
        run(OUTER, outer_step)
        finish_ring()
        wait_sends()
        many(0, ARRIVALS, lambda n: inward(n)[0].wait_send())


def one_kernel(densities, *bands):
    pairs, width = densities.shape
    rb, hw = width // 4, width // 2
    dma = pltpu.SemaphoreType.DMA
    counts = (8, 8, 8, 8, SENDS, RING, 8, 8, 4, 4, 8, 8, 4, 4, 4, 4, 12, 12)
    return pl.pallas_call(
        kernel,
        out_shape=pltpu.VMEM((width, hw), F32),
        in_specs=[
            pl.BlockSpec(memory_space=pl.ANY),
        ]
        + [pl.BlockSpec(memory_space=pltpu.VMEM)] * 4,
        out_specs=pl.BlockSpec(memory_space=pltpu.VMEM),
        scratch_shapes=[
            pltpu.VMEM((3, pairs, width), BF16),
            pltpu.VMEM((3, width, pairs), BF16),
            pltpu.VMEM((1, pairs), F32),
            pltpu.VMEM((11, width, hw), I16),
            pltpu.VMEM((SENDS, rb, hw), F32),
            pltpu.VMEM((RING, rb, hw), F32),
            pltpu.VMEM((rb, hw), F32),
            pltpu.VMEM((2, width, hw), F32),
            pltpu.VMEM((4, hw, hw), F32),
            pltpu.VMEM((hw, hw), F32),
            pltpu.VMEM((2, width, hw), I16),
            pltpu.VMEM((width, hw), I16),
            pltpu.VMEM((4, hw, hw), I16),
            pltpu.VMEM((2, hw, hw), I16),
            pltpu.VMEM((2, hw, hw), I16),
            dma,
            pltpu.SemaphoreType.REGULAR,
        ]
        + [dma((n,)) for n in counts],
        compiler_params=pltpu.CompilerParams(
            collective_id=0, has_side_effects=True, vmem_limit_bytes=58 * 2**20
        ),
    )(densities, *bands)


def solution(mesh):
    placed = (P("pair", "ga"), P("pair"), P("pair"), P(), P())
    square = mesh.shape["ga"] == PLANES and mesh.shape["pair"] == 2 * SQUARE**2
    return jax.shard_map(
        one_kernel if square else gather_all,
        mesh=mesh,
        in_specs=placed,
        out_specs=P("ga", "pair"),
        check_vma=False,
    )
```

```python
import functools
import math

import jax
import jax.numpy as jnp
from jax import lax
from jax.experimental import pallas as pl
from jax.experimental.pallas import tpu as pltpu
from jax.sharding import PartitionSpec as P

MESH = pl.DeviceIdType.MESH
PLANES, SQUARE = 4, 2
F32, BF16, I16 = jnp.float32, jnp.bfloat16, jnp.int16


def lookup(bands, table):
    levels = lax.broadcasted_iota(jnp.int32, (1, table.shape[0]), 1)
    onehot = (bands[:, None] == levels).astype(jnp.float32)
    return jnp.sum(onehot * table[None, :], axis=1)


def weights(densities, val_band, cond_band, val_energy, cond_energy):
    pairs_total = densities.shape[0] * lax.axis_size("pair")
    gap = lookup(val_band, val_energy) - lookup(cond_band, cond_energy)
    return 4.0 / (gap * math.sqrt(pairs_total))


def scale(weight, block):
    return (weight[:, None] * block.astype(jnp.float32)).astype(jnp.bfloat16)


def contract(left, right):
    return lax.dot_general(
        left, right, (((0,), (0,)), ((), ())), preferred_element_type=jnp.float32
    )


def gather_all(densities, *bands):
    scaled = scale(weights(densities, *bands), densities)
    gathered = lax.all_gather(densities, "ga", axis=1, tiled=True)
    owned = lax.psum_scatter(
        contract(gathered, scaled), "pair", scatter_dimension=0, tiled=True
    )
    return owned.T


STEPS, LOW = 816.0, -27.0


def encode(x):
    t = jnp.maximum(jnp.log2(jnp.abs(x)) * STEPS + (1.5 - LOW * STEPS), 0.0)
    return jnp.where(x < 0, -t, t).astype(jnp.int32).astype(I16)


def decode(code):
    c = code.astype(F32)
    m = jnp.exp2(jnp.abs(c) * (1 / STEPS) + (LOW - 1 / STEPS))
    return jnp.where(c < 0, -m, m)


TILES = (
    (0, 1, 1), (0, 0, 1), (0, 2, 0), (0, 3, 0),
    (2, 1, 0), (2, 0, 0), (3, 1, 0), (3, 0, 0),
    (1, 0, 1), (1, 2, 0), (1, 3, 0),
)
INWARD = ((0, 0), (1, 0), (0, 1), (1, 1), (0, 2), (1, 2), (1, 3), (0, 3))
ARRIVALS = 8
RING, SENDS = 8, 4
COUNT = 44
PIECES = (
    (
        5, 6, 20, 4, 11, 36, 10, 32, 21, 16, 17, 8, 7, 19, 33, 0, 23, 2, 3, 38, 18, 1, 37, 22,
        34, 30, 26, 31, 27, 28, 24, 40, 29, 42, 35, 12, 25, 43, 15, 39, 41, 13, 9, 14,
    ),
    (
        20, 7, 4, 6, 22, 32, 21, 5, 10, 33, 9, 36, 23, 38, 30, 11, 37, 40, 41, 15, 14, 31, 8, 42,
        34, 13, 28, 39, 24, 26, 18, 43, 1, 16, 27, 29, 35, 19, 25, 2, 12, 17, 3, 0,
    ),
)
INNER = (
    (
        3, 2, 1, 1, 0, 0, 1, 3, 1, 0, 2, 1, 24, 2, 1, 0, 3, 1, 0, 1, 1, 1, 1, 1,
        1, 0, 29, 0, 0, 23, 2, 0, 1, 3, 0, 0, 0, 1, 0, 1, 3, 1, 1, 2, 25, 0, 0, 1,
        0, 1, 1, 7, 0, 5, 3, 2, 0, 1, 18, 0, 22, 0, 1, 1, 0, 0, 1, 0, 0, 20, 3, 1,
        1, 0, 1, 1, 6, 2, 1, 0, 0, 1, 3, 0, 0, 0, 13, 0, 4, 0, 0, 2, 1, 28, 10, 8,
        1, 0, 12, 1, 0, 0, 1, 0, 0, 1, 1, 1, 0, 14, 1, 21, 11, 0, 9, 1, 0, 33, 0, 0,
        16, 15, 30, 1, 1, 0, 1, 19, 1, 26, 17, 27, 35, 37, 34, 31, 32, 36,
    ),
    (
        3, 2, 0, 0, 3, 0, 1, 0, 1, 2, 0, 0, 0, 3, 0, 25, 0, 2, 0, 0, 0, 0, 1, 1,
        2, 1, 0, 3, 22, 1, 0, 0, 0, 1, 0, 0, 1, 1, 3, 1, 0, 24, 0, 1, 1, 1, 2, 1,
        0, 0, 1, 0, 1, 1, 3, 0, 0, 23, 2, 1, 6, 0, 1, 1, 0, 1, 7, 1, 0, 2, 0, 1,
        1, 1, 0, 3, 2, 0, 0, 0, 1, 3, 1, 0, 1, 0, 1, 1, 1, 1, 0, 10, 1, 0, 1, 0,
        28, 8, 27, 0, 1, 14, 4, 1, 1, 0, 12, 1, 1, 11, 33, 26, 1, 0, 1, 1, 20, 9, 29, 0,
        16, 0, 5, 1, 17, 31, 32, 15, 13, 19, 21, 1, 37, 35, 18, 30, 36, 34,
    ),
)
OUTER = (
    (
        1, 8, 4, 0, 0, 1, 9, 0, 22, 10, 5, 18, 19, 6, 12, 0, 28, 23, 14, 1, 20, 7, 1, 24,
        15, 32, 21, 11, 34, 16, 26, 29, 30, 25, 36, 33, 13, 17, 27, 31, 37, 35,
    ),
    (
        0, 0, 0, 1, 1, 0, 4, 12, 5, 10, 6, 28, 18, 22, 19, 14, 1, 24, 20, 13, 11, 15, 1, 21,
        23, 32, 7, 33, 29, 8, 16, 26, 9, 25, 17, 27, 30, 36, 34, 31, 37, 35,
    ),
)
NOTHING = 63


def pick(index, values):
    result = jnp.int32(values[0])
    for n, value in enumerate(values):
        if n and value != values[0]:
            result = jnp.where(index == n, value, result)
    return result


def pick2(side, index, values):
    return jnp.where(side == 0, pick(index, values[0]), pick(index, values[1]))


def packed(side, index, codes):
    words = [
        [sum(v << (6 * i) for i, v in enumerate(c[n : n + 5])) for n in range(0, len(c), 5)]
        for c in codes
    ]
    word, place = pick2(side, lax.div(index, 5), words), lax.rem(index, 5)
    result = lax.rem(word, 64)
    for i in range(1, 5):
        word = lax.div(word, 64)
        result = jnp.where(place == i, lax.rem(word, 64), result)
    return result


def many(start, stop, body):
    def step(n, carry):
        body(n)
        return carry

    lax.fori_loop(start, stop, step, 0)


def kernel(
    dens, val_band, cond_band, val_energy, cond_energy, out, mb, st, weight, drecv, dsend, ring, acc, keep, keepd, keepg, xr, yr, yrd, xrd, din,
    load_sem, credit, in_s, in_r, mid_s, mid_r, p_s, p_r, xt_s, xt_r, yt_s, yt_r,
    yd_s, yd_r, xd_s, xd_r, zd_s, zd_r, g_s, g_r,
):
    pair, z = lax.axis_index("pair"), lax.axis_index("ga")
    c = pair % 2
    x = (pair // 2) % 2
    y = pair // 4
    h = z // 2
    X = (x + h) % 2
    Y = (y + h) % 2
    inner = (z == 1) | (z == 2)
    outer = (z == 0) | (z == 3)

    pairs, width = dens.shape
    half = pairs // 2
    rb = width // 4
    hw = width // 2
    kb = 256 if half % 256 == 0 else half
    keep_off = h * half
    give_off = (1 - h) * half

    def at(yy, xx, cc, zz):
        return ((yy * SQUARE + xx) * 2 + cc, zz)

    to_core = at(y, x, 1 - c, z)
    to_x = at(y, 1 - x, c, z)
    to_y = at(1 - y, x, c, z)
    z_mate = z + 1 - 2 * (z % 2)
    z_cross = 3 - z
    to_mate = at(y, x, c, z_mate)
    to_cross = at(y, x, c, z_cross)

    def remote(src, dst, send, recv, to):
        return pltpu.make_async_remote_copy(
            src_ref=src, dst_ref=dst, send_sem=send, recv_sem=recv,
            device_id=to, device_id_type=MESH,
        )

    def rows(k, size=rb):
        return pl.ds(pl.multiple_of(k * size, size), size)

    def part(off):
        return pl.ds(pl.multiple_of(off, half), half)

    side = (c + h) % 2

    def columns(k):
        return pl.ds(pl.multiple_of((k + 2 * h) % 4 * rb, rb), rb)

    def sides(k):
        return pl.ds(pl.multiple_of(k * hw, hw), hw)

    barrier = pltpu.get_barrier_semaphore()
    for to in (to_core, to_x, to_y, to_mate):
        pl.semaphore_signal(barrier, inc=1, device_id=to, device_id_type=MESH)

    @pl.when(inner)
    def _():
        pl.semaphore_signal(barrier, inc=1, device_id=to_cross, device_id_type=MESH)
        pl.semaphore_wait(barrier, 5)

    @pl.when(outer)
    def _():
        pl.semaphore_wait(barrier, 4)

    def slot_of(block):
        return jnp.minimum(block, 2)

    def place_of(block):
        return jnp.where(block == 3, give_off, keep_off)

    def inward(n):
        kind = pick(n, [i[0] for i in INWARD])
        k = pick(n, [i[1] for i in INWARD])
        off = jnp.where(kind == 0, keep_off, give_off)
        return remote(
            dens.at[part(off), columns(k)], mb.at[1, part(off), columns(k)],
            in_s.at[n], in_r.at[n], to_mate,
        ), kind, k, off

    def across(k):
        return remote(
            dens.at[part(give_off), columns(k + 2)], mb.at[2, part(give_off), columns(k + 2)],
            mid_s.at[k], mid_r.at[k], to_cross,
        )

    def relay(k):
        return remote(
            mb.at[1, part(give_off), columns(k)], mb.at[2, part(keep_off), columns(k)],
            mid_s.at[4 + k], mid_r.at[4 + k], to_cross,
        )

    def middle_in(n):
        block, k = 2 + n // 4, (n + 2 * (n // 4)) % 4
        place = mb.at[2, part(place_of(block)), columns(k)]
        return remote(place, place, mid_s.at[n], mid_r.at[n], to_cross), block, k

    def swap(n):
        return remote(
            dsend.at[n % SENDS], ring.at[n % RING], p_s.at[n % SENDS], p_r.at[n % RING], to_core
        )

    def xt(g, k, j):
        return remote(
            drecv.at[j, rows(k)], xr.at[g, rows(k)], xt_s.at[g * 4 + k], xt_r.at[g * 4 + k], to_x
        )

    def yt(k):
        return remote(xr.at[1 - Y, rows(k)], yr.at[rows(k)], yt_s.at[k], yt_r.at[k], to_y)

    def yd(j, kk):
        return remote(
            drecv.at[4 + j, rows(2 * (1 - Y) + kk)], yrd.at[j, rows(kk)],
            yd_s.at[j * 2 + kk], yd_r.at[j * 2 + kk], to_y,
        )

    def xd(t, kk, j):
        return remote(
            yrd.at[j, rows(kk)], xrd.at[t, rows(kk)],
            xd_s.at[t * 2 + kk], xd_r.at[t * 2 + kk], to_x,
        )

    def zd(t, kk):
        return remote(
            xrd.at[t, rows(kk)], din.at[t, rows(kk)],
            zd_s.at[t * 2 + kk], zd_r.at[t * 2 + kk], to_cross,
        )

    def grow(j, k):
        n = (j - 1) * 4 + k
        return remote(
            drecv.at[7 + j, rows(k)], drecv.at[j, rows(k)], g_s.at[n], g_r.at[n], to_mate
        )

    def transpose(slot, place, off, k):
        def step(n):
            r = pl.ds(pl.multiple_of(place + n * kb, kb), kb)
            w = weight[:, pl.ds(pl.multiple_of(off + n * kb, kb), kb)]
            t = mb[slot, r, columns(k)].T
            st[slot, rows(k), r] = (t.astype(F32) * w).astype(BF16)

        many(0, half // kb, step)

    def product(a, b, full, k, ch, put):
        @pl.when(full == 0)
        def _():
            put(jnp.dot(
                st[slot_of(a), rows(k), part(place_of(a))],
                mb[slot_of(b), part(place_of(b)), sides(ch)],
                preferred_element_type=F32,
            ))

        @pl.when(full == 1)
        def _():
            put(jnp.dot(st[a, rows(k)], mb[b, :, sides(ch)], preferred_element_type=F32))

    def kept(j, k, value):
        keep[j // 2, rows(k)] = value

    load = pltpu.make_async_copy(dens, mb.at[0], load_sem)

    @pl.when(outer)
    def _():
        many(0, ARRIVALS, lambda n: inward(n)[0].start())

    @pl.when(inner)
    def _():
        many(0, 4, lambda k: across(k).start())

    load.start()

    def level(bands, table):
        size = table.shape[0]
        column = jnp.broadcast_to(table[...].reshape(1, size), (8, size)).T[:, :1]
        found = lax.broadcasted_iota(jnp.int32, (size, pairs), 0) == bands[...].reshape(1, pairs)
        return jnp.sum(jnp.where(found, column, 0.0), axis=0, keepdims=True)

    gap = level(val_band, val_energy) - level(cond_band, cond_energy)
    weight[...] = 4.0 / (gap * math.sqrt(pairs * lax.axis_size("pair")))
    load.wait()

    def own(k):
        transpose(0, keep_off, keep_off, k)
        transpose(0, give_off, give_off, k)

    many(0, 4, own)

    def theirs(n, a, b, full, k):
        @pl.when(n >= SENDS)
        def _():
            swap(n).wait_send()

        @pl.when(n >= RING)
        def _():
            pl.semaphore_wait(credit, 1)

        def put(value):
            dsend[n % SENDS] = value

        product(a, b, full, k, 1 - c, put)
        swap(n).start()

    def settle(n, count, tile, a, b, full, k):
        swap(n).wait_recv()

        def put(value):
            acc[...] = value + ring[n % RING]

        product(a, b, full, k, c, put)

        @pl.when(n < count - RING)
        def _():
            pl.semaphore_signal(credit, inc=1, device_id=to_core, device_id_type=MESH)

        @pl.when((tile < 4) & (tile % 2 == X))
        def _():
            kept(tile, k, acc[...])

        stays = (tile >= 4) & (tile < 8) & (k // 2 == Y)

        @pl.when(stays)
        def _():
            keepd[tile - 4, rows(k % 2)] = acc[...]

        later = (tile == 9 + X) & (k // 2 == Y)

        @pl.when(later)
        def _():
            keepg[rows(k % 2)] = acc[...]

        @pl.when(jnp.logical_not(stays | later | ((tile < 4) & (tile % 2 == X))))
        def _():
            drecv[tile, rows(k)] = encode(acc[...])

            @pl.when(tile < 4)
            def _():
                xt(tile // 2, k, tile).start()

            @pl.when((tile >= 4) & (tile < 8))
            def _():
                yd(tile - 4, k % 2).start()

            @pl.when(tile >= 8)
            def _():
                grow(tile - 7, k).start()

    def finish_ring():
        many(0, SENDS, lambda n: swap(n).wait_send())

    def give_y(k):
        xt(1 - Y, k, 0).wait_recv()
        value = keep[1 - Y, rows(k)] + decode(xr[1 - Y, rows(k)])
        late = inner & (Y == 0) & (k // 2 == 0)

        @pl.when(late)
        def _():
            zd(0, k % 2).wait_recv()
            xr[1 - Y, rows(k)] = encode(value + decode(din[0, rows(k % 2)]))

        @pl.when(jnp.logical_not(late))
        def _():
            xr[1 - Y, rows(k)] = encode(value)

        yt(k).start()

    def finish(k):
        xt(Y, k, 0).wait_recv()
        yt(k).wait_recv()
        value = keep[Y, rows(k)] + decode(xr[Y, rows(k)]) + decode(yr[rows(k)])
        late = inner & (Y == 1) & (k // 2 == 1)

        @pl.when(late)
        def _():
            zd(0, k % 2).wait_recv()
            out[columns(k)] = value + decode(din[0, rows(k % 2)])

        @pl.when(jnp.logical_not(late))
        def _():
            out[columns(k)] = value

    def wait_sends():
        def step(k):
            xt(0, k, 0).wait_send()
            xt(1, k, 0).wait_send()
            yt(k).wait_send()

        many(0, 4, step)

    def run(lists, step):
        size = -(-max(map(len, lists)) // 5)
        padded = [list(l) + [NOTHING] * (5 * size - len(l)) for l in lists]
        words = [
            [sum(v << (6 * i) for i, v in enumerate(l[n : n + 5])) for n in range(0, 5 * size, 5)]
            for l in padded
        ]

        def one(i, state):
            word, counts = state
            code = lax.rem(word, 64)
            step(code, counts)
            counts = tuple(n + jnp.where(code == kind, 1, 0) for kind, n in enumerate(counts))
            return lax.div(word, 64), counts

        def five(w, counts):
            return lax.fori_loop(0, 5, one, (pick2(side, w, words), counts))[1]

        lax.fori_loop(0, size, five, (jnp.int32(0),) * 4)

    def on(condition, body):
        pl.when(condition)(body)

    def late_steps(code):
        n = code - 18
        on((n >= 0) & (n < 16) & (lax.div(n, 4) == 2 * (1 - Y) + X), lambda: give_y(lax.rem(n, 4)))
        on((code >= 34) & (code < 38), lambda: finish(code - 34))

    def at_piece(whose, n):
        code = packed(whose, n, PIECES)
        tile, k = lax.div(code, 4), lax.rem(code, 4)
        kind = pick(tile, [a * 8 + b * 2 + full for a, b, full in TILES])
        return tile, k, lax.div(kind, 8), lax.rem(lax.div(kind, 2), 4), lax.rem(kind, 2)

    def inner_step(code, counts):
        def form_theirs():
            tile, k, a, b, full = at_piece(1 - side, counts[0])
            theirs(counts[0], a, b, full, k)

        def form_own():
            tile, k, a, b, full = at_piece(side, counts[1])
            settle(counts[1], COUNT, tile, a, b, full, k)

        def from_across():
            copy, block, k = middle_in(counts[2])
            copy.wait_recv()
            transpose(2, place_of(block), keep_off, k)

        def from_outside():
            copy, kind, k, off = inward(counts[3])
            copy.wait_recv()
            on(kind == 1, lambda: relay(k).start())
            transpose(1, off, off, k)

        def yd_in():
            j, kk = lax.div(code - 4, 2), lax.rem(code - 4, 2)
            yd(j, kk).wait_recv()
            value = keepd[j, rows(kk)] + decode(yrd[j, rows(kk)])

            @pl.when(j % 2 == X)
            def _():
                keepd[j, rows(kk)] = value

            @pl.when(j % 2 != X)
            def _():
                yrd[j, rows(kk)] = encode(value)
                xd(j // 2, kk, j).start()

        def xd_in():
            t, kk = lax.div(code - 12, 2), lax.rem(code - 12, 2)
            xd(t, kk, 0).wait_recv()
            value = keepd[2 * t + X, rows(kk)] + decode(xrd[t, rows(kk)])
            xrd[t, rows(kk)] = encode(value)
            zd(t, kk).start()

        def pass_on():
            kk = code - 16
            zd(1, kk).wait_recv()
            value = keepg[rows(kk)] + decode(din[1, rows(kk)])
            drecv[9 + X, rows(2 * Y + kk)] = encode(value)
            grow(2 + X, 2 * Y + kk).start()

        on(code == 0, form_theirs)
        on(code == 1, form_own)
        on(code == 2, from_across)
        on(code == 3, from_outside)
        on((code >= 4) & (code < 12), yd_in)
        on((code >= 12) & (code < 16), xd_in)
        on((code >= 16) & (code < 18), pass_on)
        late_steps(code)

    def outer_step(code, counts):
        one = jnp.int32(1)
        on(code == 0, lambda: theirs(counts[0], 0, 0, one, counts[0]))
        on(code == 1, lambda: settle(counts[1], 4, jnp.int32(0), 0, 0, one, counts[1]))

        def arrived():
            j, k = 1 + lax.div(code - 4, 4), lax.rem(code - 4, 4)

            @pl.when(jnp.logical_not((j == 2 + X) & (k // 2 == Y)))
            def _():
                grow(j, k).wait_recv()

                @pl.when(j % 2 == X)
                def _():
                    kept(j, k, decode(drecv[j, rows(k)]))

                @pl.when(j % 2 != X)
                def _():
                    xt(j // 2, k, j).start()

        def arrived_last():
            j, k = 2 + X, 2 * Y + code - 16
            grow(j, k).wait_recv()
            kept(j, k, decode(drecv[j, rows(k)]))

        on((code >= 4) & (code < 16), arrived)
        on((code >= 16) & (code < 18), arrived_last)
        late_steps(code)

    @pl.when(inner)
    def _():
        run(INNER, inner_step)
        finish_ring()
        wait_sends()

        def ends(n):
            middle_in(n)[0].wait_send()
            yd(n // 2, n % 2).wait_send()

        many(0, 8, ends)

        def ends4(n):
            xd(n // 2, n % 2, 0).wait_send()
            zd(n // 2, n % 2).wait_send()

        many(0, 4, ends4)
        many(0, 12, lambda n: grow(1 + n // 4, n % 4).wait_send())

    @pl.when(outer)
    def _():
        run(OUTER, outer_step)
        finish_ring()
        wait_sends()
        many(0, ARRIVALS, lambda n: inward(n)[0].wait_send())


def one_kernel(densities, *bands):
    pairs, width = densities.shape
    rb, hw = width // 4, width // 2
    dma = pltpu.SemaphoreType.DMA
    counts = (8, 8, 8, 8, SENDS, RING, 8, 8, 4, 4, 8, 8, 4, 4, 4, 4, 12, 12)
    return pl.pallas_call(
        kernel,
        out_shape=pltpu.VMEM((width, hw), F32),
        in_specs=[
            pl.BlockSpec(memory_space=pl.ANY),
        ]
        + [pl.BlockSpec(memory_space=pltpu.VMEM)] * 4,
        out_specs=pl.BlockSpec(memory_space=pltpu.VMEM),
        scratch_shapes=[
            pltpu.VMEM((3, pairs, width), BF16),
            pltpu.VMEM((3, width, pairs), BF16),
            pltpu.VMEM((1, pairs), F32),
            pltpu.VMEM((11, width, hw), I16),
            pltpu.VMEM((SENDS, rb, hw), F32),
            pltpu.VMEM((RING, rb, hw), F32),
            pltpu.VMEM((rb, hw), F32),
            pltpu.VMEM((2, width, hw), F32),
            pltpu.VMEM((4, hw, hw), F32),
            pltpu.VMEM((hw, hw), F32),
            pltpu.VMEM((2, width, hw), I16),
            pltpu.VMEM((width, hw), I16),
            pltpu.VMEM((4, hw, hw), I16),
            pltpu.VMEM((2, hw, hw), I16),
            pltpu.VMEM((2, hw, hw), I16),
            dma,
            pltpu.SemaphoreType.REGULAR,
        ]
        + [dma((n,)) for n in counts],
        compiler_params=pltpu.CompilerParams(
            collective_id=0, has_side_effects=True, vmem_limit_bytes=58 * 2**20
        ),
    )(densities, *bands)


def solution(mesh):
    placed = (P("pair", "ga"), P("pair"), P("pair"), P(), P())
    square = mesh.shape["ga"] == PLANES and mesh.shape["pair"] == 2 * SQUARE**2
    return jax.shard_map(
        one_kernel if square else gather_all,
        mesh=mesh,
        in_specs=placed,
        out_specs=P("ga", "pair"),
        check_vma=False,
    )
```

```python
import functools
import math

import jax
import jax.numpy as jnp
from jax import lax
from jax.experimental import pallas as pl
from jax.experimental.pallas import tpu as pltpu
from jax.sharding import PartitionSpec as P

MESH = pl.DeviceIdType.MESH
PLANES, SQUARE = 4, 2
F32, BF16, I16 = jnp.float32, jnp.bfloat16, jnp.int16


def lookup(bands, table):
    levels = lax.broadcasted_iota(jnp.int32, (1, table.shape[0]), 1)
    onehot = (bands[:, None] == levels).astype(jnp.float32)
    return jnp.sum(onehot * table[None, :], axis=1)


def weights(densities, val_band, cond_band, val_energy, cond_energy):
    pairs_total = densities.shape[0] * lax.axis_size("pair")
    gap = lookup(val_band, val_energy) - lookup(cond_band, cond_energy)
    return 4.0 / (gap * math.sqrt(pairs_total))


def scale(weight, block):
    return (weight[:, None] * block.astype(jnp.float32)).astype(jnp.bfloat16)


def contract(left, right):
    return lax.dot_general(
        left, right, (((0,), (0,)), ((), ())), preferred_element_type=jnp.float32
    )


def gather_all(densities, *bands):
    scaled = scale(weights(densities, *bands), densities)
    gathered = lax.all_gather(densities, "ga", axis=1, tiled=True)
    owned = lax.psum_scatter(
        contract(gathered, scaled), "pair", scatter_dimension=0, tiled=True
    )
    return owned.T


STEPS, LOW = 816.0, -27.0


def encode(x):
    t = jnp.maximum(jnp.log2(jnp.abs(x)) * STEPS + (1.5 - LOW * STEPS), 0.0)
    return jnp.where(x < 0, -t, t).astype(jnp.int32).astype(I16)


def decode(code):
    c = code.astype(F32)
    m = jnp.exp2(jnp.abs(c) * (1 / STEPS) + (LOW - 1 / STEPS))
    return jnp.where(c < 0, -m, m)


TILES = (
    (0, 1, 1), (0, 0, 1), (0, 2, 0), (0, 3, 0),
    (2, 1, 0), (2, 0, 0), (3, 1, 0), (3, 0, 0),
    (1, 0, 1), (1, 2, 0), (1, 3, 0),
)
INWARD = ((0, 0), (1, 0), (0, 1), (1, 1), (0, 2), (1, 2), (1, 3), (0, 3))
ARRIVALS = 8
RING, SENDS = 8, 4
COUNT = 44
PIECES = (
    (
        7, 4, 6, 5, 11, 20, 21, 36, 37, 32, 18, 17, 22, 10, 8, 23, 16, 19, 33, 2, 3, 0, 26, 30,
        1, 38, 27, 34, 24, 31, 28, 42, 25, 29, 39, 43, 35, 15, 40, 14, 41, 9, 13, 12,
    ),
    (
        4, 5, 7, 6, 20, 21, 22, 32, 11, 37, 36, 23, 9, 8, 33, 10, 38, 30, 40, 42, 34, 15, 31, 41,
        28, 13, 14, 43, 26, 18, 27, 19, 29, 24, 2, 25, 12, 39, 17, 16, 35, 0, 1, 3,
    ),
)
INNER = (
    (
        2, 3, 1, 1, 0, 0, 1, 1, 0, 3, 2, 1, 2, 29, 1, 0, 3, 1, 0, 1, 1, 1, 1, 1,
        1, 1, 0, 0, 0, 3, 1, 2, 0, 7, 0, 0, 0, 0, 0, 0, 1, 3, 5, 1, 1, 1, 2, 0,
        0, 0, 1, 2, 0, 3, 0, 1, 1, 1, 0, 0, 0, 1, 1, 3, 0, 6, 1, 1, 2, 0, 0, 28,
        0, 1, 3, 0, 0, 0, 1, 0, 0, 1, 2, 1, 1, 0, 0, 1, 1, 8, 16, 1, 1, 10, 1, 1,
        14, 9, 4, 0, 0, 11, 37, 34, 13, 1, 0, 1, 17, 35, 0, 15, 26, 0, 0, 12, 36, 1, 1, 0,
        0, 1, 0, 27, 1, 0,
    ),
    (
        0, 0, 0, 1, 0, 3, 1, 2, 2, 0, 3, 0, 0, 3, 0, 0, 2, 0, 0, 0, 0, 1, 1, 1,
        0, 2, 0, 1, 1, 0, 0, 0, 1, 1, 3, 0, 1, 0, 1, 3, 0, 1, 1, 1, 1, 1, 2, 1,
        0, 3, 1, 2, 0, 6, 1, 0, 0, 1, 0, 7, 0, 0, 1, 1, 1, 2, 0, 3, 1, 0, 0, 1,
        2, 3, 1, 1, 0, 1, 0, 1, 0, 0, 0, 0, 10, 0, 0, 1, 1, 1, 0, 1, 0, 1, 29, 27,
        1, 0, 0, 1, 11, 0, 8, 1, 9, 14, 28, 16, 1, 1, 5, 15, 17, 1, 13, 26, 4, 12, 1, 36,
        1, 1, 35, 1, 34, 37,
    ),
    (
        1, 1, 0, 0, 1, 2, 1, 0, 2, 1, 3, 2, 1, 0, 3, 3, 1, 0, 1, 1, 1, 1, 1, 1,
        0, 1, 0, 0, 2, 1, 0, 0, 0, 6, 1, 1, 0, 1, 0, 0, 2, 3, 0, 1, 0, 3, 7, 1,
        0, 0, 1, 2, 3, 0, 1, 1, 0, 20, 0, 0, 5, 4, 0, 1, 21, 1, 3, 0, 2, 8, 0, 1,
        18, 0, 10, 1, 1, 1, 3, 0, 0, 1, 0, 2, 13, 1, 0, 14, 1, 1, 0, 9, 1, 0, 0, 19,
        1, 12, 1, 15, 11, 1, 0, 0, 0, 0, 0, 0, 1, 1, 1, 1, 0, 0, 37, 0, 0, 16, 1, 1,
        36, 0, 1, 17, 34, 35,
    ),
    (
        2, 0, 3, 0, 0, 1, 0, 1, 2, 0, 0, 0, 3, 3, 0, 0, 2, 0, 0, 0, 0, 1, 1, 0,
        0, 1, 1, 1, 2, 1, 0, 0, 0, 1, 3, 0, 1, 1, 3, 1, 0, 1, 0, 0, 1, 1, 2, 0,
        0, 1, 0, 0, 1, 6, 2, 1, 3, 0, 1, 1, 1, 1, 10, 1, 0, 2, 1, 0, 0, 1, 3, 11,
        0, 2, 0, 1, 3, 0, 0, 1, 0, 1, 1, 1, 7, 0, 1, 0, 0, 8, 1, 1, 0, 0, 0, 1,
        1, 0, 1, 14, 1, 1, 4, 5, 12, 1, 1, 9, 1, 15, 20, 0, 13, 1, 16, 18, 1, 0, 1, 17,
        19, 37, 21, 35, 36, 34,
    ),
    (
        1, 1, 0, 0, 1, 3, 3, 1, 2, 0, 2, 1, 2, 1, 0, 3, 1, 0, 1, 1, 1, 1, 0, 1,
        0, 0, 2, 3, 0, 0, 1, 7, 0, 1, 1, 0, 1, 0, 0, 1, 1, 2, 0, 0, 5, 3, 0, 0,
        1, 1, 2, 1, 1, 1, 0, 1, 3, 0, 0, 1, 0, 0, 1, 0, 3, 1, 1, 2, 0, 0, 1, 0,
        1, 3, 0, 0, 1, 4, 0, 35, 0, 2, 0, 0, 1, 1, 8, 0, 1, 1, 0, 0, 1, 0, 10, 0,
        0, 0, 1, 1, 9, 1, 1, 1, 14, 1, 34, 6, 11, 36, 0, 0, 1, 13, 15, 12, 37, 33, 16, 32,
        0, 17, 0, 31, 1, 30,
    ),
    (
        0, 0, 0, 1, 0, 2, 1, 2, 0, 0, 3, 0, 3, 3, 0, 0, 2, 0, 0, 0, 0, 1, 1, 0,
        1, 1, 1, 0, 1, 2, 1, 0, 1, 0, 3, 0, 3, 0, 0, 0, 1, 1, 2, 1, 0, 1, 0, 1,
        7, 3, 0, 2, 1, 0, 0, 0, 1, 1, 1, 0, 1, 2, 1, 0, 1, 3, 1, 0, 1, 0, 1, 1,
        33, 2, 3, 1, 0, 0, 1, 6, 1, 0, 1, 0, 1, 0, 1, 0, 1, 10, 1, 0, 0, 12, 1, 1,
        0, 13, 0, 0, 0, 1, 1, 14, 32, 1, 17, 31, 1, 8, 16, 9, 35, 37, 11, 0, 5, 15, 1, 34,
        4, 30, 1, 1, 36, 1,
    ),
    (
        1, 2, 3, 1, 0, 0, 1, 3, 1, 0, 2, 1, 2, 1, 0, 3, 1, 0, 1, 1, 0, 1, 1, 1,
        0, 0, 3, 24, 1, 1, 2, 0, 0, 0, 1, 1, 22, 0, 1, 1, 1, 0, 1, 0, 0, 0, 2, 6,
        1, 3, 0, 7, 0, 23, 2, 1, 0, 3, 0, 0, 1, 25, 0, 0, 8, 3, 5, 0, 1, 2, 1, 0,
        1, 1, 0, 1, 1, 0, 13, 4, 3, 1, 0, 9, 0, 1, 0, 2, 1, 10, 0, 0, 1, 0, 14, 1,
        1, 1, 0, 0, 11, 0, 0, 1, 0, 0, 1, 0, 1, 0, 12, 0, 1, 0, 1, 15, 0, 16, 1, 1,
        17, 37, 35, 1, 36, 34,
    ),
    (
        2, 3, 0, 0, 0, 1, 0, 1, 2, 0, 3, 0, 0, 3, 0, 0, 2, 0, 0, 0, 0, 1, 0, 0,
        1, 1, 2, 1, 22, 0, 0, 3, 1, 1, 0, 25, 0, 23, 0, 1, 0, 1, 6, 1, 2, 1, 1, 0,
        3, 2, 1, 3, 1, 0, 7, 1, 1, 1, 1, 1, 0, 0, 1, 0, 0, 1, 2, 0, 0, 3, 0, 1,
        10, 1, 1, 14, 0, 12, 2, 3, 0, 0, 0, 0, 1, 0, 0, 0, 1, 0, 1, 11, 1, 1, 8, 1,
        1, 15, 1, 4, 1, 1, 1, 13, 9, 1, 1, 1, 0, 5, 0, 16, 1, 1, 24, 1, 0, 1, 1, 37,
        0, 35, 17, 36, 0, 34,
    ),
)
OUTER = (
    (
        5, 4, 0, 1, 0, 6, 0, 14, 0, 1, 1, 16, 10, 1, 34, 11, 26, 7, 29, 12, 36, 17, 27, 15,
        28, 37, 35, 13,
    ),
    (
        4, 10, 5, 1, 0, 0, 14, 1, 0, 12, 6, 1, 35, 15, 28, 13, 0, 16, 26, 1, 36, 11, 29, 37,
        17, 27, 34, 7,
    ),
    (
        0, 9, 1, 0, 0, 0, 5, 4, 8, 1, 1, 19, 1, 18, 14, 21, 6, 7, 20, 15, 16, 34, 12, 36,
        13, 35, 17, 37,
    ),
    (
        0, 4, 1, 18, 1, 14, 1, 0, 0, 9, 19, 12, 5, 1, 13, 6, 0, 20, 21, 15, 7, 16, 8, 17,
        34, 37, 36, 35,
    ),
    (
        8, 9, 0, 1, 0, 0, 0, 5, 1, 10, 4, 1, 6, 14, 1, 34, 11, 32, 16, 30, 7, 15, 33, 37,
        35, 36, 17, 31,
    ),
    (
        0, 1, 1, 9, 1, 4, 10, 0, 0, 14, 0, 15, 32, 5, 8, 33, 6, 34, 1, 11, 17, 31, 16, 30,
        7, 35, 36, 37,
    ),
    (
        1, 8, 0, 9, 0, 5, 4, 1, 0, 1, 22, 0, 1, 6, 7, 23, 11, 25, 10, 24, 12, 13, 34, 16,
        17, 36, 37, 35,
    ),
    (
        0, 0, 1, 1, 1, 4, 9, 22, 0, 6, 5, 1, 0, 16, 10, 36, 13, 12, 8, 7, 24, 11, 23, 35,
        34, 25, 17, 37,
    ),
)
NOTHING = 63


def pick(index, values):
    result = jnp.int32(values[0])
    for n, value in enumerate(values):
        if n and value != values[0]:
            result = jnp.where(index == n, value, result)
    return result


def pick2(side, index, values):
    return jnp.where(side == 0, pick(index, values[0]), pick(index, values[1]))


def packed(side, index, codes):
    words = [
        [sum(v << (6 * i) for i, v in enumerate(c[n : n + 5])) for n in range(0, len(c), 5)]
        for c in codes
    ]
    word, place = pick2(side, lax.div(index, 5), words), lax.rem(index, 5)
    result = lax.rem(word, 64)
    for i in range(1, 5):
        word = lax.div(word, 64)
        result = jnp.where(place == i, lax.rem(word, 64), result)
    return result


def many(start, stop, body):
    def step(n, carry):
        body(n)
        return carry

    lax.fori_loop(start, stop, step, 0)


def kernel(
    dens, val_band, cond_band, val_energy, cond_energy, out, mb, st, weight, drecv, dsend, ring, acc, keep, keepd, keepg, xr, yr, yrd, xrd, din,
    load_sem, credit, in_s, in_r, mid_s, mid_r, p_s, p_r, xt_s, xt_r, yt_s, yt_r,
    yd_s, yd_r, xd_s, xd_r, zd_s, zd_r, g_s, g_r,
):
    pair, z = lax.axis_index("pair"), lax.axis_index("ga")
    c = pair % 2
    x = (pair // 2) % 2
    y = pair // 4
    h = z // 2
    X = (x + h) % 2
    Y = (y + h) % 2
    inner = (z == 1) | (z == 2)
    outer = (z == 0) | (z == 3)

    pairs, width = dens.shape
    half = pairs // 2
    rb = width // 4
    hw = width // 2
    kb = 256 if half % 256 == 0 else half
    keep_off = h * half
    give_off = (1 - h) * half

    def at(yy, xx, cc, zz):
        return ((yy * SQUARE + xx) * 2 + cc, zz)

    to_core = at(y, x, 1 - c, z)
    to_x = at(y, 1 - x, c, z)
    to_y = at(1 - y, x, c, z)
    z_mate = z + 1 - 2 * (z % 2)
    z_cross = 3 - z
    to_mate = at(y, x, c, z_mate)
    to_cross = at(y, x, c, z_cross)

    def remote(src, dst, send, recv, to):
        return pltpu.make_async_remote_copy(
            src_ref=src, dst_ref=dst, send_sem=send, recv_sem=recv,
            device_id=to, device_id_type=MESH,
        )

    def rows(k, size=rb):
        return pl.ds(pl.multiple_of(k * size, size), size)

    def part(off):
        return pl.ds(pl.multiple_of(off, half), half)

    side = (c + h) % 2

    def columns(k):
        return pl.ds(pl.multiple_of((k + 2 * h) % 4 * rb, rb), rb)

    def sides(k):
        return pl.ds(pl.multiple_of(k * hw, hw), hw)

    barrier = pltpu.get_barrier_semaphore()
    for to in (to_core, to_x, to_y, to_mate):
        pl.semaphore_signal(barrier, inc=1, device_id=to, device_id_type=MESH)

    @pl.when(inner)
    def _():
        pl.semaphore_signal(barrier, inc=1, device_id=to_cross, device_id_type=MESH)
        pl.semaphore_wait(barrier, 5)

    @pl.when(outer)
    def _():
        pl.semaphore_wait(barrier, 4)

    def slot_of(block):
        return jnp.minimum(block, 2)

    def place_of(block):
        return jnp.where(block == 3, give_off, keep_off)

    def inward(n):
        kind = pick(n, [i[0] for i in INWARD])
        k = pick(n, [i[1] for i in INWARD])
        off = jnp.where(kind == 0, keep_off, give_off)
        return remote(
            dens.at[part(off), columns(k)], mb.at[1, part(off), columns(k)],
            in_s.at[n], in_r.at[n], to_mate,
        ), kind, k, off

    def across(k):
        return remote(
            dens.at[part(give_off), columns(k + 2)], mb.at[2, part(give_off), columns(k + 2)],
            mid_s.at[k], mid_r.at[k], to_cross,
        )

    def relay(k):
        return remote(
            mb.at[1, part(give_off), columns(k)], mb.at[2, part(keep_off), columns(k)],
            mid_s.at[4 + k], mid_r.at[4 + k], to_cross,
        )

    def middle_in(n):
        block, k = 2 + n // 4, (n + 2 * (n // 4)) % 4
        place = mb.at[2, part(place_of(block)), columns(k)]
        return remote(place, place, mid_s.at[n], mid_r.at[n], to_cross), block, k

    def swap(n):
        return remote(
            dsend.at[n % SENDS], ring.at[n % RING], p_s.at[n % SENDS], p_r.at[n % RING], to_core
        )

    def xt(g, k, j):
        return remote(
            drecv.at[j, rows(k)], xr.at[g, rows(k)], xt_s.at[g * 4 + k], xt_r.at[g * 4 + k], to_x
        )

    def yt(k):
        return remote(xr.at[1 - Y, rows(k)], yr.at[rows(k)], yt_s.at[k], yt_r.at[k], to_y)

    def yd(j, kk):
        return remote(
            drecv.at[4 + j, rows(2 * (1 - Y) + kk)], yrd.at[j, rows(kk)],
            yd_s.at[j * 2 + kk], yd_r.at[j * 2 + kk], to_y,
        )

    def xd(t, kk, j):
        return remote(
            yrd.at[j, rows(kk)], xrd.at[t, rows(kk)],
            xd_s.at[t * 2 + kk], xd_r.at[t * 2 + kk], to_x,
        )

    def zd(t, kk):
        return remote(
            xrd.at[t, rows(kk)], din.at[t, rows(kk)],
            zd_s.at[t * 2 + kk], zd_r.at[t * 2 + kk], to_cross,
        )

    def grow(j, k):
        n = (j - 1) * 4 + k
        return remote(
            drecv.at[7 + j, rows(k)], drecv.at[j, rows(k)], g_s.at[n], g_r.at[n], to_mate
        )

    def transpose(slot, place, off, k):
        def step(n):
            r = pl.ds(pl.multiple_of(place + n * kb, kb), kb)
            w = weight[:, pl.ds(pl.multiple_of(off + n * kb, kb), kb)]
            t = mb[slot, r, columns(k)].T
            st[slot, rows(k), r] = (t.astype(F32) * w).astype(BF16)

        many(0, half // kb, step)

    def product(a, b, full, k, ch, put):
        @pl.when(full == 0)
        def _():
            put(jnp.dot(
                st[slot_of(a), rows(k), part(place_of(a))],
                mb[slot_of(b), part(place_of(b)), sides(ch)],
                preferred_element_type=F32,
            ))

        @pl.when(full == 1)
        def _():
            put(jnp.dot(st[a, rows(k)], mb[b, :, sides(ch)], preferred_element_type=F32))

    def kept(j, k, value):
        keep[j // 2, rows(k)] = value

    load = pltpu.make_async_copy(dens, mb.at[0], load_sem)

    @pl.when(outer)
    def _():
        many(0, ARRIVALS, lambda n: inward(n)[0].start())

    @pl.when(inner)
    def _():
        many(0, 4, lambda k: across(k).start())

    load.start()

    def level(bands, table):
        size = table.shape[0]
        column = jnp.broadcast_to(table[...].reshape(1, size), (8, size)).T[:, :1]
        found = lax.broadcasted_iota(jnp.int32, (size, pairs), 0) == bands[...].reshape(1, pairs)
        return jnp.sum(jnp.where(found, column, 0.0), axis=0, keepdims=True)

    gap = level(val_band, val_energy) - level(cond_band, cond_energy)
    weight[...] = 4.0 / (gap * math.sqrt(pairs * lax.axis_size("pair")))
    load.wait()

    def own(k):
        transpose(0, keep_off, keep_off, k)
        transpose(0, give_off, give_off, k)

    many(0, 4, own)

    def theirs(n, a, b, full, k):
        @pl.when(n >= SENDS)
        def _():
            swap(n).wait_send()

        @pl.when(n >= RING)
        def _():
            pl.semaphore_wait(credit, 1)

        def put(value):
            dsend[n % SENDS] = value

        product(a, b, full, k, 1 - c, put)
        swap(n).start()

    def settle(n, count, tile, a, b, full, k):
        swap(n).wait_recv()

        def put(value):
            acc[...] = value + ring[n % RING]

        product(a, b, full, k, c, put)

        @pl.when(n < count - RING)
        def _():
            pl.semaphore_signal(credit, inc=1, device_id=to_core, device_id_type=MESH)

        @pl.when((tile < 4) & (tile % 2 == X))
        def _():
            kept(tile, k, acc[...])

        stays = (tile >= 4) & (tile < 8) & (k // 2 == Y)

        @pl.when(stays)
        def _():
            keepd[tile - 4, rows(k % 2)] = acc[...]

        later = (tile == 9 + X) & (k // 2 == Y)

        @pl.when(later)
        def _():
            keepg[rows(k % 2)] = acc[...]

        @pl.when(jnp.logical_not(stays | later | ((tile < 4) & (tile % 2 == X))))
        def _():
            drecv[tile, rows(k)] = encode(acc[...])

            @pl.when(tile < 4)
            def _():
                xt(tile // 2, k, tile).start()

            @pl.when((tile >= 4) & (tile < 8))
            def _():
                yd(tile - 4, k % 2).start()

            @pl.when(tile >= 8)
            def _():
                grow(tile - 7, k).start()

    def finish_ring():
        many(0, SENDS, lambda n: swap(n).wait_send())

    def give_y(k):
        xt(1 - Y, k, 0).wait_recv()
        value = keep[1 - Y, rows(k)] + decode(xr[1 - Y, rows(k)])
        late = inner & (Y == 0) & (k // 2 == 0)

        @pl.when(late)
        def _():
            zd(0, k % 2).wait_recv()
            xr[1 - Y, rows(k)] = encode(value + decode(din[0, rows(k % 2)]))

        @pl.when(jnp.logical_not(late))
        def _():
            xr[1 - Y, rows(k)] = encode(value)

        yt(k).start()

    def finish(k):
        xt(Y, k, 0).wait_recv()
        yt(k).wait_recv()
        value = keep[Y, rows(k)] + decode(xr[Y, rows(k)]) + decode(yr[rows(k)])
        late = inner & (Y == 1) & (k // 2 == 1)

        @pl.when(late)
        def _():
            zd(0, k % 2).wait_recv()
            out[columns(k)] = value + decode(din[0, rows(k % 2)])

        @pl.when(jnp.logical_not(late))
        def _():
            out[columns(k)] = value

    def wait_sends():
        def step(k):
            xt(0, k, 0).wait_send()
            xt(1, k, 0).wait_send()
            yt(k).wait_send()

        many(0, 4, step)

    def run(lists, step):
        size = -(-max(map(len, lists)) // 5)
        padded = [list(l) + [NOTHING] * (5 * size - len(l)) for l in lists]
        words = [
            [sum(v << (6 * i) for i, v in enumerate(l[n : n + 5])) for n in range(0, 5 * size, 5)]
            for l in padded
        ]

        flat = [word for l in words for word in l]
        role = 4 * X + 2 * Y + side

        def one(i, state):
            word, counts = state
            code = lax.rem(word, 64)
            step(code, counts)
            counts = tuple(n + jnp.where(code == kind, 1, 0) for kind, n in enumerate(counts))
            return lax.div(word, 64), counts

        def five(w, counts):
            return lax.fori_loop(0, 5, one, (pick(role * size + w, flat), counts))[1]

        lax.fori_loop(0, size, five, (jnp.int32(0),) * 4)

    def on(condition, body):
        pl.when(condition)(body)

    def late_steps(code):
        n = code - 18
        on((n >= 0) & (n < 16) & (lax.div(n, 4) == 2 * (1 - Y) + X), lambda: give_y(lax.rem(n, 4)))
        on((code >= 34) & (code < 38), lambda: finish(code - 34))

    def at_piece(whose, n):
        code = packed(whose, n, PIECES)
        tile, k = lax.div(code, 4), lax.rem(code, 4)
        kind = pick(tile, [a * 8 + b * 2 + full for a, b, full in TILES])
        return tile, k, lax.div(kind, 8), lax.rem(lax.div(kind, 2), 4), lax.rem(kind, 2)

    def inner_step(code, counts):
        def form_theirs():
            tile, k, a, b, full = at_piece(1 - side, counts[0])
            theirs(counts[0], a, b, full, k)

        def form_own():
            tile, k, a, b, full = at_piece(side, counts[1])
            settle(counts[1], COUNT, tile, a, b, full, k)

        def from_across():
            copy, block, k = middle_in(counts[2])
            copy.wait_recv()
            transpose(2, place_of(block), keep_off, k)

        def from_outside():
            copy, kind, k, off = inward(counts[3])
            copy.wait_recv()
            on(kind == 1, lambda: relay(k).start())
            transpose(1, off, off, k)

        def yd_in():
            j, kk = lax.div(code - 4, 2), lax.rem(code - 4, 2)
            yd(j, kk).wait_recv()
            value = keepd[j, rows(kk)] + decode(yrd[j, rows(kk)])

            @pl.when(j % 2 == X)
            def _():
                keepd[j, rows(kk)] = value

            @pl.when(j % 2 != X)
            def _():
                yrd[j, rows(kk)] = encode(value)
                xd(j // 2, kk, j).start()

        def xd_in():
            t, kk = lax.div(code - 12, 2), lax.rem(code - 12, 2)
            xd(t, kk, 0).wait_recv()
            value = keepd[2 * t + X, rows(kk)] + decode(xrd[t, rows(kk)])
            xrd[t, rows(kk)] = encode(value)
            zd(t, kk).start()

        def pass_on():
            kk = code - 16
            zd(1, kk).wait_recv()
            value = keepg[rows(kk)] + decode(din[1, rows(kk)])
            drecv[9 + X, rows(2 * Y + kk)] = encode(value)
            grow(2 + X, 2 * Y + kk).start()

        on(code == 0, form_theirs)
        on(code == 1, form_own)
        on(code == 2, from_across)
        on(code == 3, from_outside)
        on((code >= 4) & (code < 12), yd_in)
        on((code >= 12) & (code < 16), xd_in)
        on((code >= 16) & (code < 18), pass_on)
        late_steps(code)

    def outer_step(code, counts):
        one = jnp.int32(1)
        on(code == 0, lambda: theirs(counts[0], 0, 0, one, counts[0]))
        on(code == 1, lambda: settle(counts[1], 4, jnp.int32(0), 0, 0, one, counts[1]))

        def arrived():
            j, k = 1 + lax.div(code - 4, 4), lax.rem(code - 4, 4)

            @pl.when(jnp.logical_not((j == 2 + X) & (k // 2 == Y)))
            def _():
                grow(j, k).wait_recv()

                @pl.when(j % 2 == X)
                def _():
                    kept(j, k, decode(drecv[j, rows(k)]))

                @pl.when(j % 2 != X)
                def _():
                    xt(j // 2, k, j).start()

        def arrived_last():
            j, k = 2 + X, 2 * Y + code - 16
            grow(j, k).wait_recv()
            kept(j, k, decode(drecv[j, rows(k)]))

        on((code >= 4) & (code < 16), arrived)
        on((code >= 16) & (code < 18), arrived_last)
        late_steps(code)

    @pl.when(inner)
    def _():
        run(INNER, inner_step)
        finish_ring()
        wait_sends()

        def ends(n):
            middle_in(n)[0].wait_send()
            yd(n // 2, n % 2).wait_send()

        many(0, 8, ends)

        def ends4(n):
            xd(n // 2, n % 2, 0).wait_send()
            zd(n // 2, n % 2).wait_send()

        many(0, 4, ends4)
        many(0, 12, lambda n: grow(1 + n // 4, n % 4).wait_send())

    @pl.when(outer)
    def _():
        run(OUTER, outer_step)
        finish_ring()
        wait_sends()
        many(0, ARRIVALS, lambda n: inward(n)[0].wait_send())


def one_kernel(densities, *bands):
    pairs, width = densities.shape
    rb, hw = width // 4, width // 2
    dma = pltpu.SemaphoreType.DMA
    counts = (8, 8, 8, 8, SENDS, RING, 8, 8, 4, 4, 8, 8, 4, 4, 4, 4, 12, 12)
    return pl.pallas_call(
        kernel,
        out_shape=pltpu.VMEM((width, hw), F32),
        in_specs=[
            pl.BlockSpec(memory_space=pl.ANY),
        ]
        + [pl.BlockSpec(memory_space=pltpu.VMEM)] * 4,
        out_specs=pl.BlockSpec(memory_space=pltpu.VMEM),
        scratch_shapes=[
            pltpu.VMEM((3, pairs, width), BF16),
            pltpu.VMEM((3, width, pairs), BF16),
            pltpu.VMEM((1, pairs), F32),
            pltpu.VMEM((11, width, hw), I16),
            pltpu.VMEM((SENDS, rb, hw), F32),
            pltpu.VMEM((RING, rb, hw), F32),
            pltpu.VMEM((rb, hw), F32),
            pltpu.VMEM((2, width, hw), F32),
            pltpu.VMEM((4, hw, hw), F32),
            pltpu.VMEM((hw, hw), F32),
            pltpu.VMEM((2, width, hw), I16),
            pltpu.VMEM((width, hw), I16),
            pltpu.VMEM((4, hw, hw), I16),
            pltpu.VMEM((2, hw, hw), I16),
            pltpu.VMEM((2, hw, hw), I16),
            dma,
            pltpu.SemaphoreType.REGULAR,
        ]
        + [dma((n,)) for n in counts],
        compiler_params=pltpu.CompilerParams(
            collective_id=0, has_side_effects=True, vmem_limit_bytes=58 * 2**20
        ),
    )(densities, *bands)


def solution(mesh):
    placed = (P("pair", "ga"), P("pair"), P("pair"), P(), P())
    square = mesh.shape["ga"] == PLANES and mesh.shape["pair"] == 2 * SQUARE**2
    return jax.shard_map(
        one_kernel if square else gather_all,
        mesh=mesh,
        in_specs=placed,
        out_specs=P("ga", "pair"),
        check_vma=False,
    )
```

```python
import functools
import math

import jax
import jax.numpy as jnp
from jax import lax
from jax.experimental import pallas as pl
from jax.experimental.pallas import tpu as pltpu
from jax.sharding import PartitionSpec as P

MESH = pl.DeviceIdType.MESH
PLANES, SQUARE = 4, 2
F32, BF16, I16 = jnp.float32, jnp.bfloat16, jnp.int16


def lookup(bands, table):
    levels = lax.broadcasted_iota(jnp.int32, (1, table.shape[0]), 1)
    onehot = (bands[:, None] == levels).astype(jnp.float32)
    return jnp.sum(onehot * table[None, :], axis=1)


def weights(densities, val_band, cond_band, val_energy, cond_energy):
    pairs_total = densities.shape[0] * lax.axis_size("pair")
    gap = lookup(val_band, val_energy) - lookup(cond_band, cond_energy)
    return 4.0 / (gap * math.sqrt(pairs_total))


def scale(weight, block):
    return (weight[:, None] * block.astype(jnp.float32)).astype(jnp.bfloat16)


def contract(left, right):
    return lax.dot_general(
        left, right, (((0,), (0,)), ((), ())), preferred_element_type=jnp.float32
    )


def gather_all(densities, *bands):
    scaled = scale(weights(densities, *bands), densities)
    gathered = lax.all_gather(densities, "ga", axis=1, tiled=True)
    owned = lax.psum_scatter(
        contract(gathered, scaled), "pair", scatter_dimension=0, tiled=True
    )
    return owned.T


STEPS, LOW = 816.0, -27.0


def encode(x):
    t = jnp.maximum(jnp.log2(jnp.abs(x)) * STEPS + (1.5 - LOW * STEPS), 0.0)
    return jnp.where(x < 0, -t, t).astype(jnp.int32).astype(I16)


def decode(code):
    c = code.astype(F32)
    m = jnp.exp2(jnp.abs(c) * (1 / STEPS) + (LOW - 1 / STEPS))
    return jnp.where(c < 0, -m, m)


TILES = (
    (0, 1, 1), (0, 0, 1), (0, 2, 0), (0, 3, 0),
    (2, 1, 0), (2, 0, 0), (3, 1, 0), (3, 0, 0),
    (1, 0, 1), (1, 2, 0), (1, 3, 0),
)
INWARD = ((1, 0), (0, 0), (0, 1), (1, 1), (0, 2), (1, 2), (1, 3), (0, 3))
ARRIVALS = 8
RING, SENDS = 8, 4
COUNT = 44
PIECES = (
    (
        5, 6, 4, 11, 21, 7, 10, 20, 18, 22, 36, 37, 32, 17, 16, 23, 19, 1, 33, 3, 0, 8, 26, 38,
        30, 27, 34, 31, 2, 9, 24, 28, 39, 25, 43, 35, 29, 42, 40, 41, 14, 15, 13, 12,
    ),
    (
        4, 5, 7, 6, 32, 21, 22, 20, 11, 9, 23, 33, 37, 36, 38, 41, 31, 14, 42, 40, 15, 12, 8, 34,
        13, 28, 30, 43, 19, 39, 27, 26, 10, 24, 25, 18, 29, 1, 17, 35, 16, 2, 3, 0,
    ),
)
INNER = (
    (
        0, 1, 0, 2, 3, 1, 0, 2, 0, 1, 1, 1, 1, 2, 3, 1, 3, 0, 1, 0, 1, 1, 6, 7,
        1, 0, 1, 0, 1, 1, 1, 3, 2, 0, 1, 0, 1, 1, 0, 1, 3, 0, 0, 1, 0, 2, 0, 1,
        1, 2, 0, 3, 1, 0, 0, 0, 1, 0, 0, 0, 1, 28, 0, 1, 3, 0, 1, 0, 2, 0, 0, 1,
        1, 1, 3, 0, 0, 0, 1, 35, 0, 5, 2, 1, 1, 0, 1, 0, 1, 4, 1, 8, 0, 10, 1, 1,
        0, 1, 0, 12, 1, 1, 14, 9, 11, 15, 1, 0, 0, 13, 0, 1, 16, 27, 36, 34, 0, 0, 0, 37,
        29, 0, 0, 17, 1, 26,
    ),
    (
        3, 1, 2, 0, 0, 1, 0, 1, 2, 0, 1, 0, 3, 0, 0, 0, 3, 2, 0, 1, 0, 0, 0, 2,
        0, 0, 1, 3, 0, 0, 0, 0, 0, 1, 0, 1, 0, 1, 7, 6, 1, 0, 3, 1, 2, 1, 0, 0,
        1, 1, 1, 2, 1, 0, 1, 3, 1, 0, 1, 0, 1, 0, 1, 0, 2, 0, 1, 0, 1, 1, 1, 0,
        3, 1, 1, 29, 3, 0, 2, 0, 1, 0, 1, 1, 0, 0, 0, 0, 0, 1, 1, 0, 27, 1, 10, 26,
        0, 1, 1, 1, 0, 8, 17, 14, 1, 0, 11, 9, 28, 1, 16, 1, 15, 1, 5, 1, 4, 13, 1, 12,
        1, 37, 36, 35, 1, 34,
    ),
    (
        0, 1, 0, 2, 1, 0, 2, 3, 0, 1, 1, 1, 1, 2, 1, 3, 0, 3, 1, 0, 1, 0, 3, 0,
        1, 2, 0, 1, 1, 0, 0, 6, 1, 4, 0, 1, 1, 0, 1, 0, 3, 1, 1, 1, 0, 1, 2, 1,
        2, 3, 7, 1, 1, 19, 0, 0, 21, 0, 0, 0, 0, 1, 1, 0, 3, 0, 18, 1, 1, 2, 0, 1,
        1, 0, 0, 1, 1, 0, 3, 0, 0, 5, 8, 12, 9, 0, 1, 13, 0, 0, 1, 2, 20, 14, 11, 10,
        1, 1, 0, 1, 15, 1, 0, 0, 0, 0, 0, 1, 0, 0, 1, 0, 0, 36, 1, 0, 16, 1, 0, 35,
        1, 1, 1, 37, 17, 34,
    ),
    (
        1, 0, 0, 2, 1, 0, 2, 1, 0, 1, 3, 0, 3, 0, 0, 0, 3, 2, 0, 1, 0, 1, 0, 2,
        0, 1, 1, 0, 1, 0, 0, 1, 0, 3, 0, 2, 1, 0, 3, 0, 0, 0, 1, 0, 0, 0, 6, 2,
        0, 3, 0, 1, 0, 1, 1, 0, 7, 1, 1, 1, 0, 0, 1, 1, 1, 2, 1, 3, 0, 1, 1, 11,
        2, 0, 1, 3, 1, 0, 0, 1, 1, 1, 0, 0, 1, 0, 10, 0, 1, 1, 1, 0, 1, 1, 0, 1,
        9, 0, 5, 1, 8, 15, 1, 14, 1, 1, 1, 13, 19, 1, 0, 35, 0, 16, 0, 4, 1, 12, 20, 1,
        17, 34, 21, 37, 18, 36,
    ),
    (
        0, 2, 1, 0, 3, 1, 0, 0, 2, 1, 1, 1, 1, 2, 3, 1, 3, 0, 1, 0, 1, 1, 3, 2,
        0, 0, 1, 0, 0, 1, 0, 0, 0, 1, 1, 1, 1, 7, 1, 3, 1, 1, 0, 1, 1, 1, 2, 2,
        1, 0, 0, 0, 0, 1, 1, 3, 0, 0, 4, 0, 1, 3, 0, 0, 1, 0, 0, 2, 1, 0, 34, 5,
        1, 0, 3, 0, 0, 0, 6, 1, 0, 0, 0, 2, 1, 0, 0, 8, 0, 0, 1, 1, 0, 1, 1, 35,
        10, 1, 0, 9, 13, 0, 1, 1, 0, 14, 0, 0, 1, 1, 0, 11, 15, 37, 12, 1, 1, 32, 16, 1,
        33, 36, 17, 31, 1, 30,
    ),
    (
        1, 0, 3, 2, 0, 1, 0, 1, 2, 0, 1, 0, 3, 0, 0, 0, 3, 2, 0, 1, 0, 0, 0, 34,
        0, 3, 2, 1, 1, 1, 0, 0, 0, 1, 0, 1, 0, 2, 0, 0, 0, 1, 0, 3, 0, 0, 1, 0,
        1, 2, 1, 3, 0, 0, 1, 1, 7, 1, 0, 1, 0, 1, 1, 1, 2, 32, 1, 1, 3, 1, 1, 0,
        0, 1, 0, 3, 0, 2, 0, 1, 1, 0, 0, 1, 0, 13, 1, 1, 1, 1, 0, 35, 1, 0, 6, 12,
        0, 1, 0, 1, 1, 37, 0, 31, 30, 17, 8, 1, 10, 33, 1, 16, 14, 0, 9, 1, 11, 5, 0, 1,
        4, 1, 1, 1, 15, 36,
    ),
    (
        3, 0, 1, 0, 1, 2, 0, 0, 2, 1, 1, 1, 1, 2, 3, 1, 23, 3, 0, 1, 0, 0, 1, 1,
        3, 2, 0, 4, 0, 1, 1, 1, 0, 0, 0, 1, 1, 1, 1, 0, 1, 0, 25, 3, 0, 2, 22, 1,
        1, 1, 3, 2, 0, 0, 1, 24, 1, 0, 0, 0, 0, 1, 0, 1, 0, 6, 3, 8, 1, 7, 0, 1,
        5, 1, 1, 0, 1, 2, 1, 0, 1, 3, 0, 0, 12, 9, 0, 0, 0, 1, 0, 2, 13, 0, 1, 0,
        1, 0, 0, 0, 1, 1, 0, 0, 1, 0, 1, 0, 0, 10, 11, 1, 15, 14, 0, 0, 1, 16, 1, 17,
        1, 1, 37, 35, 36, 34,
    ),
    (
        2, 3, 1, 0, 0, 1, 2, 0, 1, 0, 1, 0, 0, 0, 3, 22, 0, 3, 2, 0, 1, 0, 1, 0,
        0, 0, 0, 3, 24, 0, 1, 1, 25, 2, 0, 0, 1, 0, 1, 3, 0, 1, 0, 0, 1, 2, 1, 1,
        0, 0, 0, 1, 2, 1, 1, 0, 3, 0, 0, 1, 0, 1, 2, 0, 1, 1, 0, 0, 0, 23, 1, 3,
        6, 1, 7, 1, 1, 3, 0, 2, 0, 1, 0, 1, 1, 0, 1, 1, 1, 1, 0, 1, 0, 1, 0, 11,
        5, 1, 13, 1, 9, 10, 0, 14, 1, 8, 1, 0, 1, 1, 0, 1, 1, 0, 15, 4, 36, 12, 17, 1,
        1, 16, 34, 35, 37, 0,
    ),
)
OUTER = (
    (
        0, 1, 0, 6, 1, 10, 0, 1, 1, 34, 4, 15, 7, 5, 28, 11, 14, 12, 35, 13, 29, 36, 37, 0,
        16, 26, 17, 27,
    ),
    (
        10, 1, 0, 13, 0, 5, 1, 14, 0, 12, 0, 4, 11, 15, 28, 29, 34, 17, 27, 1, 6, 36, 35, 16,
        26, 1, 37, 7,
    ),
    (
        0, 5, 1, 0, 18, 9, 0, 1, 0, 4, 6, 1, 20, 8, 7, 19, 1, 15, 21, 14, 12, 16, 36, 13,
        17, 34, 37, 35,
    ),
    (
        0, 1, 0, 9, 0, 1, 4, 5, 8, 1, 19, 0, 14, 1, 13, 20, 6, 12, 15, 18, 21, 7, 17, 37,
        35, 16, 36, 34,
    ),
    (
        4, 1, 1, 0, 0, 5, 9, 10, 6, 0, 1, 1, 0, 7, 11, 15, 8, 33, 36, 37, 14, 34, 32, 35,
        16, 30, 17, 31,
    ),
    (
        4, 0, 0, 9, 0, 1, 8, 5, 1, 0, 10, 6, 14, 15, 11, 1, 32, 35, 33, 17, 31, 1, 34, 16,
        30, 36, 7, 37,
    ),
    (
        1, 8, 0, 0, 4, 1, 1, 0, 0, 1, 5, 10, 23, 7, 6, 22, 24, 25, 16, 36, 11, 9, 13, 12,
        17, 37, 34, 35,
    ),
    (
        0, 0, 4, 1, 0, 5, 1, 0, 1, 23, 12, 22, 9, 10, 6, 1, 13, 17, 11, 8, 35, 7, 37, 24,
        16, 36, 34, 25,
    ),
)
NOTHING = 63


def pick(index, values):
    result = jnp.int32(values[0])
    for n, value in enumerate(values):
        if n and value != values[0]:
            result = jnp.where(index == n, value, result)
    return result


def pick2(side, index, values):
    return jnp.where(side == 0, pick(index, values[0]), pick(index, values[1]))


def packed(side, index, codes):
    words = [
        [sum(v << (6 * i) for i, v in enumerate(c[n : n + 5])) for n in range(0, len(c), 5)]
        for c in codes
    ]
    word, place = pick2(side, lax.div(index, 5), words), lax.rem(index, 5)
    result = lax.rem(word, 64)
    for i in range(1, 5):
        word = lax.div(word, 64)
        result = jnp.where(place == i, lax.rem(word, 64), result)
    return result


def many(start, stop, body):
    def step(n, carry):
        body(n)
        return carry

    lax.fori_loop(start, stop, step, 0)


def kernel(
    dens, val_band, cond_band, val_energy, cond_energy, out, mb, st, weight, drecv, dsend, ring, acc, keep, keepd, keepg, xr, yr, yrd, xrd, din,
    load_sem, credit, in_s, in_r, mid_s, mid_r, p_s, p_r, xt_s, xt_r, yt_s, yt_r,
    yd_s, yd_r, xd_s, xd_r, zd_s, zd_r, g_s, g_r,
):
    pair, z = lax.axis_index("pair"), lax.axis_index("ga")
    c = pair % 2
    x = (pair // 2) % 2
    y = pair // 4
    h = z // 2
    X = (x + h) % 2
    Y = (y + h) % 2
    inner = (z == 1) | (z == 2)
    outer = (z == 0) | (z == 3)

    pairs, width = dens.shape
    half = pairs // 2
    rb = width // 4
    hw = width // 2
    kb = 256 if half % 256 == 0 else half
    keep_off = h * half
    give_off = (1 - h) * half

    def at(yy, xx, cc, zz):
        return ((yy * SQUARE + xx) * 2 + cc, zz)

    to_core = at(y, x, 1 - c, z)
    to_x = at(y, 1 - x, c, z)
    to_y = at(1 - y, x, c, z)
    z_mate = z + 1 - 2 * (z % 2)
    z_cross = 3 - z
    to_mate = at(y, x, c, z_mate)
    to_cross = at(y, x, c, z_cross)

    def remote(src, dst, send, recv, to):
        return pltpu.make_async_remote_copy(
            src_ref=src, dst_ref=dst, send_sem=send, recv_sem=recv,
            device_id=to, device_id_type=MESH,
        )

    def rows(k, size=rb):
        return pl.ds(pl.multiple_of(k * size, size), size)

    def part(off):
        return pl.ds(pl.multiple_of(off, half), half)

    side = (c + h) % 2

    def columns(k):
        return pl.ds(pl.multiple_of((k + 2 * h) % 4 * rb, rb), rb)

    def sides(k):
        return pl.ds(pl.multiple_of(k * hw, hw), hw)

    barrier = pltpu.get_barrier_semaphore()
    for to in (to_core, to_x, to_y, to_mate):
        pl.semaphore_signal(barrier, inc=1, device_id=to, device_id_type=MESH)

    @pl.when(inner)
    def _():
        pl.semaphore_signal(barrier, inc=1, device_id=to_cross, device_id_type=MESH)
        pl.semaphore_wait(barrier, 5)

    @pl.when(outer)
    def _():
        pl.semaphore_wait(barrier, 4)

    def slot_of(block):
        return jnp.minimum(block, 2)

    def place_of(block):
        return jnp.where(block == 3, give_off, keep_off)

    def inward(n):
        kind = pick(n, [i[0] for i in INWARD])
        k = pick(n, [i[1] for i in INWARD])
        off = jnp.where(kind == 0, keep_off, give_off)
        return remote(
            dens.at[part(off), columns(k)], mb.at[1, part(off), columns(k)],
            in_s.at[n], in_r.at[n], to_mate,
        ), kind, k, off

    def across(k):
        return remote(
            dens.at[part(give_off), columns(k + 2)], mb.at[2, part(give_off), columns(k + 2)],
            mid_s.at[k], mid_r.at[k], to_cross,
        )

    def relay(k):
        return remote(
            mb.at[1, part(give_off), columns(k)], mb.at[2, part(keep_off), columns(k)],
            mid_s.at[4 + k], mid_r.at[4 + k], to_cross,
        )

    def middle_in(n):
        block, k = 2 + n // 4, (n + 2 * (n // 4)) % 4
        place = mb.at[2, part(place_of(block)), columns(k)]
        return remote(place, place, mid_s.at[n], mid_r.at[n], to_cross), block, k

    def swap(n):
        return remote(
            dsend.at[n % SENDS], ring.at[n % RING], p_s.at[n % SENDS], p_r.at[n % RING], to_core
        )

    def xt(g, k, j):
        return remote(
            drecv.at[j, rows(k)], xr.at[g, rows(k)], xt_s.at[g * 4 + k], xt_r.at[g * 4 + k], to_x
        )

    def yt(k):
        return remote(xr.at[1 - Y, rows(k)], yr.at[rows(k)], yt_s.at[k], yt_r.at[k], to_y)

    def yd(j, kk):
        return remote(
            drecv.at[4 + j, rows(2 * (1 - Y) + kk)], yrd.at[j, rows(kk)],
            yd_s.at[j * 2 + kk], yd_r.at[j * 2 + kk], to_y,
        )

    def xd(t, kk, j):
        return remote(
            yrd.at[j, rows(kk)], xrd.at[t, rows(kk)],
            xd_s.at[t * 2 + kk], xd_r.at[t * 2 + kk], to_x,
        )

    def zd(t, kk):
        return remote(
            xrd.at[t, rows(kk)], din.at[t, rows(kk)],
            zd_s.at[t * 2 + kk], zd_r.at[t * 2 + kk], to_cross,
        )

    def grow(j, k):
        n = (j - 1) * 4 + k
        return remote(
            drecv.at[7 + j, rows(k)], drecv.at[j, rows(k)], g_s.at[n], g_r.at[n], to_mate
        )

    def transpose(slot, place, off, k):
        def step(n):
            r = pl.ds(pl.multiple_of(place + n * kb, kb), kb)
            w = weight[:, pl.ds(pl.multiple_of(off + n * kb, kb), kb)]
            t = mb[slot, r, columns(k)].T
            st[slot, rows(k), r] = (t.astype(F32) * w).astype(BF16)

        many(0, half // kb, step)

    def product(a, b, full, k, ch, put):
        @pl.when(full == 0)
        def _():
            put(jnp.dot(
                st[slot_of(a), rows(k), part(place_of(a))],
                mb[slot_of(b), part(place_of(b)), sides(ch)],
                preferred_element_type=F32,
            ))

        @pl.when(full == 1)
        def _():
            put(jnp.dot(st[a, rows(k)], mb[b, :, sides(ch)], preferred_element_type=F32))

    def kept(j, k, value):
        keep[j // 2, rows(k)] = value

    load = pltpu.make_async_copy(dens, mb.at[0], load_sem)

    @pl.when(outer)
    def _():
        many(0, ARRIVALS, lambda n: inward(n)[0].start())

    @pl.when(inner)
    def _():
        many(0, 4, lambda k: across(k).start())

    load.start()

    def level(bands, table):
        size = table.shape[0]
        column = jnp.broadcast_to(table[...].reshape(1, size), (8, size)).T[:, :1]
        found = lax.broadcasted_iota(jnp.int32, (size, pairs), 0) == bands[...].reshape(1, pairs)
        return jnp.sum(jnp.where(found, column, 0.0), axis=0, keepdims=True)

    gap = level(val_band, val_energy) - level(cond_band, cond_energy)
    weight[...] = 4.0 / (gap * math.sqrt(pairs * lax.axis_size("pair")))
    load.wait()

    def own(k):
        transpose(0, keep_off, keep_off, k)
        transpose(0, give_off, give_off, k)

    many(0, 4, own)

    def theirs(n, a, b, full, k):
        @pl.when(n >= SENDS)
        def _():
            swap(n).wait_send()

        @pl.when(n >= RING)
        def _():
            pl.semaphore_wait(credit, 1)

        def put(value):
            dsend[n % SENDS] = value

        product(a, b, full, k, 1 - c, put)
        swap(n).start()

    def settle(n, count, tile, a, b, full, k):
        swap(n).wait_recv()

        def put(value):
            acc[...] = value + ring[n % RING]

        product(a, b, full, k, c, put)

        @pl.when(n < count - RING)
        def _():
            pl.semaphore_signal(credit, inc=1, device_id=to_core, device_id_type=MESH)

        @pl.when((tile < 4) & (tile % 2 == X))
        def _():
            kept(tile, k, acc[...])

        stays = (tile >= 4) & (tile < 8) & (k // 2 == Y)

        @pl.when(stays)
        def _():
            keepd[tile - 4, rows(k % 2)] = acc[...]

        later = (tile == 9 + X) & (k // 2 == Y)

        @pl.when(later)
        def _():
            keepg[rows(k % 2)] = acc[...]

        @pl.when(jnp.logical_not(stays | later | ((tile < 4) & (tile % 2 == X))))
        def _():
            drecv[tile, rows(k)] = encode(acc[...])

            @pl.when(tile < 4)
            def _():
                xt(tile // 2, k, tile).start()

            @pl.when((tile >= 4) & (tile < 8))
            def _():
                yd(tile - 4, k % 2).start()

            @pl.when(tile >= 8)
            def _():
                grow(tile - 7, k).start()

    def finish_ring():
        many(0, SENDS, lambda n: swap(n).wait_send())

    def give_y(k):
        xt(1 - Y, k, 0).wait_recv()
        value = keep[1 - Y, rows(k)] + decode(xr[1 - Y, rows(k)])
        late = inner & (Y == 0) & (k // 2 == 0)

        @pl.when(late)
        def _():
            zd(0, k % 2).wait_recv()
            xr[1 - Y, rows(k)] = encode(value + decode(din[0, rows(k % 2)]))

        @pl.when(jnp.logical_not(late))
        def _():
            xr[1 - Y, rows(k)] = encode(value)

        yt(k).start()

    def finish(k):
        xt(Y, k, 0).wait_recv()
        yt(k).wait_recv()
        value = keep[Y, rows(k)] + decode(xr[Y, rows(k)]) + decode(yr[rows(k)])
        late = inner & (Y == 1) & (k // 2 == 1)

        @pl.when(late)
        def _():
            zd(0, k % 2).wait_recv()
            out[columns(k)] = value + decode(din[0, rows(k % 2)])

        @pl.when(jnp.logical_not(late))
        def _():
            out[columns(k)] = value

    def wait_sends():
        def step(k):
            xt(0, k, 0).wait_send()
            xt(1, k, 0).wait_send()
            yt(k).wait_send()

        many(0, 4, step)

    def run(lists, step):
        size = -(-max(map(len, lists)) // 5)
        padded = [list(l) + [NOTHING] * (5 * size - len(l)) for l in lists]
        words = [
            [sum(v << (6 * i) for i, v in enumerate(l[n : n + 5])) for n in range(0, 5 * size, 5)]
            for l in padded
        ]

        flat = [word for l in words for word in l]
        role = 4 * X + 2 * Y + side

        def one(i, state):
            word, counts = state
            code = lax.rem(word, 64)
            step(code, counts)
            counts = tuple(n + jnp.where(code == kind, 1, 0) for kind, n in enumerate(counts))
            return lax.div(word, 64), counts

        def five(w, counts):
            return lax.fori_loop(0, 5, one, (pick(role * size + w, flat), counts))[1]

        lax.fori_loop(0, size, five, (jnp.int32(0),) * 4)

    def on(condition, body):
        pl.when(condition)(body)

    def late_steps(code):
        n = code - 18
        on((n >= 0) & (n < 16) & (lax.div(n, 4) == 2 * (1 - Y) + X), lambda: give_y(lax.rem(n, 4)))
        on((code >= 34) & (code < 38), lambda: finish(code - 34))

    def at_piece(whose, n):
        code = packed(whose, n, PIECES)
        tile, k = lax.div(code, 4), lax.rem(code, 4)
        kind = pick(tile, [a * 8 + b * 2 + full for a, b, full in TILES])
        return tile, k, lax.div(kind, 8), lax.rem(lax.div(kind, 2), 4), lax.rem(kind, 2)

    def inner_step(code, counts):
        def form_theirs():
            tile, k, a, b, full = at_piece(1 - side, counts[0])
            theirs(counts[0], a, b, full, k)

        def form_own():
            tile, k, a, b, full = at_piece(side, counts[1])
            settle(counts[1], COUNT, tile, a, b, full, k)

        def from_across():
            copy, block, k = middle_in(counts[2])
            copy.wait_recv()
            transpose(2, place_of(block), keep_off, k)

        def from_outside():
            copy, kind, k, off = inward(counts[3])
            copy.wait_recv()
            on(kind == 1, lambda: relay(k).start())
            transpose(1, off, off, k)

        def yd_in():
            j, kk = lax.div(code - 4, 2), lax.rem(code - 4, 2)
            yd(j, kk).wait_recv()
            value = keepd[j, rows(kk)] + decode(yrd[j, rows(kk)])

            @pl.when(j % 2 == X)
            def _():
                keepd[j, rows(kk)] = value

            @pl.when(j % 2 != X)
            def _():
                yrd[j, rows(kk)] = encode(value)
                xd(j // 2, kk, j).start()

        def xd_in():
            t, kk = lax.div(code - 12, 2), lax.rem(code - 12, 2)
            xd(t, kk, 0).wait_recv()
            value = keepd[2 * t + X, rows(kk)] + decode(xrd[t, rows(kk)])
            xrd[t, rows(kk)] = encode(value)
            zd(t, kk).start()

        def pass_on():
            kk = code - 16
            zd(1, kk).wait_recv()
            value = keepg[rows(kk)] + decode(din[1, rows(kk)])
            drecv[9 + X, rows(2 * Y + kk)] = encode(value)
            grow(2 + X, 2 * Y + kk).start()

        on(code == 0, form_theirs)
        on(code == 1, form_own)
        on(code == 2, from_across)
        on(code == 3, from_outside)
        on((code >= 4) & (code < 12), yd_in)
        on((code >= 12) & (code < 16), xd_in)
        on((code >= 16) & (code < 18), pass_on)
        late_steps(code)

    def outer_step(code, counts):
        one = jnp.int32(1)
        on(code == 0, lambda: theirs(counts[0], 0, 0, one, counts[0]))
        on(code == 1, lambda: settle(counts[1], 4, jnp.int32(0), 0, 0, one, counts[1]))

        def arrived():
            j, k = 1 + lax.div(code - 4, 4), lax.rem(code - 4, 4)

            @pl.when(jnp.logical_not((j == 2 + X) & (k // 2 == Y)))
            def _():
                grow(j, k).wait_recv()

                @pl.when(j % 2 == X)
                def _():
                    kept(j, k, decode(drecv[j, rows(k)]))

                @pl.when(j % 2 != X)
                def _():
                    xt(j // 2, k, j).start()

        def arrived_last():
            j, k = 2 + X, 2 * Y + code - 16
            grow(j, k).wait_recv()
            kept(j, k, decode(drecv[j, rows(k)]))

        on((code >= 4) & (code < 16), arrived)
        on((code >= 16) & (code < 18), arrived_last)
        late_steps(code)

    @pl.when(inner)
    def _():
        run(INNER, inner_step)
        finish_ring()
        wait_sends()

        def ends(n):
            middle_in(n)[0].wait_send()
            yd(n // 2, n % 2).wait_send()

        many(0, 8, ends)

        def ends4(n):
            xd(n // 2, n % 2, 0).wait_send()
            zd(n // 2, n % 2).wait_send()

        many(0, 4, ends4)
        many(0, 12, lambda n: grow(1 + n // 4, n % 4).wait_send())

    @pl.when(outer)
    def _():
        run(OUTER, outer_step)
        finish_ring()
        wait_sends()
        many(0, ARRIVALS, lambda n: inward(n)[0].wait_send())


def one_kernel(densities, *bands):
    pairs, width = densities.shape
    rb, hw = width // 4, width // 2
    dma = pltpu.SemaphoreType.DMA
    counts = (8, 8, 8, 8, SENDS, RING, 8, 8, 4, 4, 8, 8, 4, 4, 4, 4, 12, 12)
    return pl.pallas_call(
        kernel,
        out_shape=pltpu.VMEM((width, hw), F32),
        in_specs=[
            pl.BlockSpec(memory_space=pl.ANY),
        ]
        + [pl.BlockSpec(memory_space=pltpu.VMEM)] * 4,
        out_specs=pl.BlockSpec(memory_space=pltpu.VMEM),
        scratch_shapes=[
            pltpu.VMEM((3, pairs, width), BF16),
            pltpu.VMEM((3, width, pairs), BF16),
            pltpu.VMEM((1, pairs), F32),
            pltpu.VMEM((11, width, hw), I16),
            pltpu.VMEM((SENDS, rb, hw), F32),
            pltpu.VMEM((RING, rb, hw), F32),
            pltpu.VMEM((rb, hw), F32),
            pltpu.VMEM((2, width, hw), F32),
            pltpu.VMEM((4, hw, hw), F32),
            pltpu.VMEM((hw, hw), F32),
            pltpu.VMEM((2, width, hw), I16),
            pltpu.VMEM((width, hw), I16),
            pltpu.VMEM((4, hw, hw), I16),
            pltpu.VMEM((2, hw, hw), I16),
            pltpu.VMEM((2, hw, hw), I16),
            dma,
            pltpu.SemaphoreType.REGULAR,
        ]
        + [dma((n,)) for n in counts],
        compiler_params=pltpu.CompilerParams(
            collective_id=0, has_side_effects=True, vmem_limit_bytes=58 * 2**20
        ),
    )(densities, *bands)


def solution(mesh):
    placed = (P("pair", "ga"), P("pair"), P("pair"), P(), P())
    square = mesh.shape["ga"] == PLANES and mesh.shape["pair"] == 2 * SQUARE**2
    return jax.shard_map(
        one_kernel if square else gather_all,
        mesh=mesh,
        in_specs=placed,
        out_specs=P("ga", "pair"),
        check_vma=False,
    )
```
